32 devices in a mesh: batch: 2 (over x), col: 4 (over z), row: 4 (over y, core).
Axes of the slice: x: 2, y: 2, z: 4, core: 2. Of those that a mesh axis runs over, the one named last changes fastest.
Arguments:
- images: bfloat16 [32, 512, 512, 3], P('batch', 'row', 'col'), parts along dimension 0
- w_down1: bfloat16 [4, 4, 3, 64], replicated
- b_down1: float32 [64], replicated
- w_conv1: bfloat16 [3, 3, 64, 64], replicated
- b_conv1: float32 [64], replicated
- w_down2: bfloat16 [4, 4, 64, 128], replicated
- b_down2: float32 [128], replicated
- w_conv2: bfloat16 [3, 3, 128, 128], replicated
- b_conv2: float32 [128], replicated
- w_down3: bfloat16 [4, 4, 128, 256], replicated
- b_down3: float32 [256], replicated
- w_conv3: bfloat16 [3, 3, 256, 256], replicated
- b_conv3: float32 [256], replicated
Outputs:
- output: bfloat16 [32, 64, 64, 256], P('batch', 'row', 'col'), parts along dimension 0
There are 2 independent parts. The reference program is written for one: setup_inputs(seed, part) draws one part's arguments, and reference() takes and returns one part's arrays. A program takes and returns all parts, laid end to end along the dimension named above; an argument that names none is the same for every part.
All inputs are finite; a program needn't handle non-finite values.
Results may differ from the reference program's by a relative error of at most 0.00425.
Values are sent between devices in bfloat16 or wider.
A program may use at most 1 GiB of HBM per device.

```python
import jax
import jax.numpy as jnp
from jax import lax

NUM_IMAGES = 16
IMG_HEIGHT = 512
IMG_WIDTH = 512
CH_IN = 3
CH_ONE = 64
CH_TWO = 128
CH_THREE = 256


def setup_inputs(seed: int = 0, part: int = 0) -> dict:
    key_list = jax.random.split(jax.random.key(seed), 13)
    image_key = jax.random.fold_in(key_list[0], part)
    images = jax.random.normal(image_key, (NUM_IMAGES, IMG_HEIGHT, IMG_WIDTH, CH_IN), jnp.float32)
    drawn_args = {'images': images.astype(jnp.bfloat16)}
    widths = [CH_IN, CH_ONE, CH_TWO, CH_THREE]
    for stage_idx in range(3):
        c_in = widths[stage_idx]
        c_out = widths[stage_idx + 1]
        key_base = 1 + 4 * stage_idx
        w_down = jax.random.normal(key_list[key_base], (4, 4, c_in, c_out), jnp.float32) * (2.0 / (16 * c_in)) ** 0.5
        b_down = 0.25 * jax.random.normal(key_list[key_base + 1], (c_out,), jnp.float32)
        w_conv = jax.random.normal(key_list[key_base + 2], (3, 3, c_out, c_out), jnp.float32) * (2.0 / (9 * c_out)) ** 0.5
        b_conv = 0.25 * jax.random.normal(key_list[key_base + 3], (c_out,), jnp.float32)
        suffix = str(stage_idx + 1)
        drawn_args['w_down' + suffix] = w_down.astype(jnp.bfloat16)
        drawn_args['b_down' + suffix] = b_down
        drawn_args['w_conv' + suffix] = w_conv.astype(jnp.bfloat16)
        drawn_args['b_conv' + suffix] = b_conv
    return drawn_args


def conv_relu(act_in, weight, bias_vec, stride):
    summed = lax.conv_general_dilated(act_in.astype(jnp.float32), weight.astype(jnp.float32), (stride, stride), ((1, 1), (1, 1)), dimension_numbers=('NHWC', 'HWIO', 'NHWC'))
    return jax.nn.relu(summed + bias_vec).astype(jnp.bfloat16)


def reference(images, w_down1, b_down1, w_conv1, b_conv1, w_down2, b_down2, w_conv2, b_conv2, w_down3, b_down3, w_conv3, b_conv3):
    params = [(w_down1, b_down1, w_conv1, b_conv1), (w_down2, b_down2, w_conv2, b_conv2), (w_down3, b_down3, w_conv3, b_conv3)]

    def encode(one_image):
        act_tile = one_image[None]
        for w_down, b_down, w_conv, b_conv in params:
            act_tile = conv_relu(act_tile, w_down, b_down, 2)
            act_tile = conv_relu(act_tile, w_conv, b_conv, 1)
        return act_tile[0]

    return lax.map(encode, images)
```

```python
import functools

import jax
import jax.numpy as jnp
from jax import lax
from jax.experimental import pallas as pl
from jax.experimental.pallas import tpu as pltpu
from jax.sharding import PartitionSpec as P

MESH = pl.DeviceIdType.MESH
F32 = jnp.float32
BF16 = jnp.bfloat16


def body(rows, cols, x_ref, wd1, bd1, wc1, bc1, wd2, bd2, wc2, bc2, wd3, bd3, wc3, bc3, out_ref,
         top, bot, tt, send_l, send_r, recv_l, recv_r, y1, z1, y2, z2, y3, ssem, rsem):
    r = lax.axis_index('row')
    c = lax.axis_index('col')
    has_up, has_dn = r > 0, r < rows - 1
    has_lf, has_rt = c > 0, c < cols - 1

    neighbours = []
    for dr in (-1, 0, 1):
        for dc in (-1, 0, 1):
            if dr == 0 and dc == 0:
                continue
            there = None
            if dr:
                there = has_up if dr < 0 else has_dn
            if dc:
                side = has_lf if dc < 0 else has_rt
                there = side if there is None else jnp.logical_and(there, side)
            neighbours.append((dr, dc, there))

    def device(dr, dc):
        return {'row': r + dr, 'col': c + dc}

    barrier = pltpu.get_barrier_semaphore()
    for dr, dc, there in neighbours:
        @pl.when(there)
        def _():
            pl.semaphore_signal(barrier, inc=1, device_id=device(dr, dc), device_id_type=MESH)
    n_r = has_up.astype(jnp.int32) + has_dn.astype(jnp.int32)
    n_c = has_lf.astype(jnp.int32) + has_rt.astype(jnp.int32)
    pl.semaphore_wait(barrier, (n_r + 1) * (n_c + 1) - 1)

    def remote(src, dst, k, dr, dc):
        return pltpu.make_async_remote_copy(src_ref=src, dst_ref=dst, send_sem=ssem.at[k], recv_sem=rsem.at[k],
                                            device_id=device(dr, dc), device_id_type=MESH)

    to_dn = remote(x_ref.at[:, 112:128], top, 0, 1, 0)
    to_up = remote(x_ref.at[:, 0:16], bot, 1, -1, 0)

    @pl.when(has_dn)
    def _():
        to_dn.start()

    @pl.when(has_up)
    def _():
        to_up.start()

    @pl.when(jnp.logical_not(has_up))
    def _():
        top[...] = jnp.zeros_like(top)

    @pl.when(jnp.logical_not(has_dn))
    def _():
        bot[...] = jnp.zeros_like(bot)

    def put(cu, g, stack):
        t = jnp.transpose(stack.astype(F32))
        lanes = slice(g * 128, g * 128 + 128)
        tt[cu, 13:141, lanes] = t
        send_l[cu, :, lanes] = t[0:16].astype(BF16)
        send_r[cu, :, lanes] = t[112:128].astype(BF16)

    def inner(ch, _):
        for u in range(4):
            for g in (1, 2, 3):
                h0 = 32 * g + u - 13
                pieces = [x_ref[ch, h0 + 4 * k] for k in range(8)]
                put(ch * 4 + u, g, jnp.concatenate(pieces, axis=0))
        return 0

    lax.fori_loop(0, 3, inner, 0)

    @pl.when(has_up)
    def _():
        to_up.wait_send()
        remote(x_ref.at[:, 112:128], top, 0, 1, 0).wait_recv()

    @pl.when(has_dn)
    def _():
        to_dn.wait_send()
        remote(x_ref.at[:, 0:16], bot, 1, -1, 0).wait_recv()

    def outer(ch, _):
        for u in range(4):
            for g in (0, 4):
                pieces = []
                for k in range(8):
                    h = 32 * g + u - 13 + 4 * k
                    if h < 0:
                        pieces.append(top[ch, h + 16])
                    elif h < 128:
                        pieces.append(x_ref[ch, h])
                    elif h < 144:
                        pieces.append(bot[ch, h - 128])
                    else:
                        pieces.append(jnp.zeros((16, 128), BF16))
                put(ch * 4 + u, g, jnp.concatenate(pieces, axis=0))
        return 0

    lax.fori_loop(0, 3, outer, 0)

    to_lf = remote(send_l, recv_r, 2, 0, -1)
    to_rt = remote(send_r, recv_l, 3, 0, 1)

    @pl.when(has_lf)
    def _():
        to_lf.start()

    @pl.when(has_rt)
    def _():
        to_rt.start()

    def dots(pairs):
        acc = None
        for lhs, w in pairs:
            d = jnp.dot(lhs, w, preferred_element_type=F32)
            acc = d if acc is None else acc + d
        return acc

    def finish(acc, bias, shape):
        return jnp.maximum(acc + bias[...], 0.0).astype(BF16).reshape(shape)

    def down1(k, _):
        win = tt[:, pl.ds(pl.multiple_of(8 * k, 8), 16), :]
        for e in range(2):
            xt = jnp.transpose(win[:, 4 * e:4 * e + 8].reshape(96, 640))
            xb = jnp.concatenate([xt.astype(BF16), jnp.zeros((640, 32), BF16)], axis=1)
            lhs = jnp.concatenate([xb[0:608], xb[16:624]], axis=1)
            y1[2 * k + e] = finish(dots([(lhs, wd1[...])]), bd1, (38, 16, 256))
        return 0

    lax.fori_loop(2, 17, down1, 0)

    @pl.when(has_lf)
    def _():
        to_lf.wait_send()
        to_rt.wait_recv()

    @pl.when(has_rt)
    def _():
        to_rt.wait_send()
        to_lf.wait_recv()

    @pl.when(jnp.logical_not(has_lf))
    def _():
        recv_l[...] = jnp.zeros_like(recv_l)

    @pl.when(jnp.logical_not(has_rt))
    def _():
        recv_r[...] = jnp.zeros_like(recv_r)

    tt[:, 0:13, :] = recv_l[...].astype(F32)[:, 3:16]
    tt[:, 141:157, :] = recv_r[...].astype(F32)
    lax.fori_loop(0, 2, down1, 0)
    lax.fori_loop(17, 19, down1, 0)

    def clear(ref, there, index):
        @pl.when(jnp.logical_not(there))
        def _():
            ref[index] = jnp.zeros_like(ref[index])

    every = slice(None)
    clear(y1, has_up, (every, slice(0, 3)))
    clear(y1, has_dn, (every, slice(35, 38)))
    clear(y1, has_lf, (slice(0, 3),))
    clear(y1, has_rt, (slice(35, 38),))

    def conv1(b, _):
        pairs = [(y1[b + dw, dh:dh + 37].reshape(592, 256), wc1[dw, dh]) for dw in range(2) for dh in range(2)]
        z1[b] = finish(dots(pairs), bc1, (37, 16, 256))
        return 0

    lax.fori_loop(0, 37, conv1, 0)
    clear(z1, has_up, (every, slice(0, 2)))
    clear(z1, has_up, (every, slice(2, 3), every, slice(0, 128)))
    clear(z1, has_dn, (every, slice(35, 37)))
    clear(z1, has_dn, (every, slice(34, 35), every, slice(128, 256)))
    clear(z1, has_lf, (slice(0, 2),))
    clear(z1, has_rt, (slice(35, 37),))
    for half in (0, 128):
        clear(z1, has_lf, (slice(2, 3), every, every, slice(half, half + 64)))
        clear(z1, has_rt, (slice(34, 35), every, every, slice(half + 64, half + 128)))

    def down2(p, _):
        pairs = [(z1[2 * p + dw, dh:dh + 36].reshape(576, 256), wd2[dw, dh]) for dw in range(3) for dh in range(2)]
        y2[p] = finish(dots(pairs), bd2, (36, 16, 256))
        return 0

    lax.fori_loop(0, 18, down2, 0)
    clear(y2, has_up, (every, slice(0, 2)))
    clear(y2, has_dn, (every, slice(34, 36)))
    clear(y2, has_lf, (slice(0, 1),))
    clear(y2, has_rt, (slice(17, 18),))

    def conv2(q, _):
        pairs = [(y2[q + dw, dh:dh + 34].reshape(544, 256), wc2[dw, dh]) for dw in range(2) for dh in range(3)]
        z2[q] = finish(dots(pairs), bc2, (34, 16, 256))
        return 0

    lax.fori_loop(0, 17, conv2, 0)
    clear(z2, has_up, (every, slice(0, 1)))
    clear(z2, has_dn, (every, slice(33, 34)))
    clear(z2, has_lf, (slice(0, 1), every, every, slice(0, 128)))
    clear(z2, has_rt, (slice(16, 17), every, every, slice(128, 256)))

    def down3(k, _):
        pairs = []
        for dw in range(2):
            for dh in range(4):
                lhs = [z2[2 * k + e + dw, dh + 2 * i] for e in range(2) for i in range(16)]
                pairs.append((jnp.concatenate(lhs, axis=0), wd3[dw, dh]))
        y3[pl.ds(2 * k + 1, 2), 1:17] = finish(dots(pairs), bd3, (2, 16, 16, 256))
        return 0

    lax.fori_loop(0, 8, down3, 0)

    def edge(d):
        return slice(1, 17) if d == 0 else (slice(16, 17) if d > 0 else slice(1, 2))

    def place(d):
        return slice(1, 17) if d == 0 else (slice(0, 1) if d > 0 else slice(17, 18))

    copies = []
    for k, (dr, dc, there) in enumerate(neighbours):
        copies.append(remote(y3.at[edge(dc), edge(dr)], y3.at[place(dc), place(dr)], 4 + k, dr, dc))

        @pl.when(there)
        def _():
            copies[k].start()
    clear(y3, has_up, (every, slice(0, 1)))
    clear(y3, has_dn, (every, slice(17, 18)))
    clear(y3, has_lf, (slice(0, 1),))
    clear(y3, has_rt, (slice(17, 18),))
    for k, (dr, dc, there) in enumerate(neighbours):
        @pl.when(there)
        def _():
            copies[k].wait_send()
            copies[7 - k].wait_recv()

    def conv3(k, _):
        pairs = []
        for dw in range(3):
            for dh in range(3):
                lhs = y3[pl.ds(2 * k + dw, 2), dh:dh + 16].reshape(512, 256)
                pairs.append((lhs, wc3[dh, dw]))
        out_ref[pl.ds(2 * k, 2)] = finish(dots(pairs), bc3, (2, 16, 16, 256))
        return 0

    lax.fori_loop(0, 8, conv3, 0)


def taps(w, axis, e, step, size):
    pads = [(0, 0)] * w.ndim
    pads[axis] = (step * e, size - w.shape[axis] - step * e)
    return jnp.pad(w, pads)


def solution(mesh):
    rows, cols = mesh.shape['row'], mesh.shape['col']

    def local(images, w_down1, b_down1, w_conv1, b_conv1, w_down2, b_down2, w_conv2, b_conv2, w_down3, b_down3, w_conv3, b_conv3):
        x = jnp.transpose(images, (3, 1, 0, 2))
        w = jnp.concatenate([taps(taps(w_down1, 0, eh, 2, 8), 1, ew, 2, 8) for eh in range(2) for ew in range(2)], axis=3)
        w = w.reshape(2, 4, 8, 3, 256).transpose(0, 3, 1, 2, 4).reshape(2, 96, 256)
        wd1 = jnp.pad(w, ((0, 0), (0, 32), (0, 0))).reshape(256, 256)
        w = jnp.concatenate([taps(taps(w_conv1, 0, eh, 1, 4), 1, ew, 1, 4) for eh in range(2) for ew in range(2)], axis=3)
        wc1 = w.reshape(2, 2, 2, 2, 64, 256).transpose(2, 0, 1, 3, 4, 5).reshape(2, 2, 256, 256)
        w = jnp.concatenate([taps(w_down2, 1, ew, 2, 6) for ew in range(2)], axis=3)
        wd2 = w.reshape(2, 2, 3, 2, 64, 256).transpose(2, 0, 1, 3, 4, 5).reshape(3, 2, 256, 256)
        w = jnp.concatenate([taps(w_conv2, 1, ew, 1, 4) for ew in range(2)], axis=3)
        wc2 = w.reshape(3, 2, 2, 128, 256).transpose(1, 0, 2, 3, 4).reshape(2, 3, 256, 256)
        wd3 = w_down3.reshape(4, 2, 2, 128, 256).transpose(1, 0, 2, 3, 4).reshape(2, 4, 256, 256)

        def bias(b, times):
            return jnp.tile(b, times).reshape(1, 256)

        vmem = pl.BlockSpec(memory_space=pltpu.VMEM)
        out = pl.pallas_call(
            functools.partial(body, rows, cols),
            out_shape=jax.ShapeDtypeStruct((16, 16, 16, 256), BF16),
            in_specs=[vmem] * 13,
            out_specs=vmem,
            scratch_shapes=[
                pltpu.VMEM((3, 16, 16, 128), BF16),
                pltpu.VMEM((3, 16, 16, 128), BF16),
                pltpu.VMEM((12, 160, 640), F32),
                pltpu.VMEM((12, 16, 640), BF16),
                pltpu.VMEM((12, 16, 640), BF16),
                pltpu.VMEM((12, 16, 640), BF16),
                pltpu.VMEM((12, 16, 640), BF16),
                pltpu.VMEM((38, 38, 16, 256), BF16),
                pltpu.VMEM((37, 37, 16, 256), BF16),
                pltpu.VMEM((18, 36, 16, 256), BF16),
                pltpu.VMEM((17, 34, 16, 256), BF16),
                pltpu.VMEM((18, 18, 16, 256), BF16),
                pltpu.SemaphoreType.DMA((12,)),
                pltpu.SemaphoreType.DMA((12,)),
            ],
            compiler_params=pltpu.CompilerParams(collective_id=0, has_side_effects=True, vmem_limit_bytes=66_000_000),
            name='encoder',
        )(x, wd1, bias(b_down1, 4), wc1, bias(b_conv1, 4), wd2, bias(b_down2, 2), wc2, bias(b_conv2, 2),
          wd3, bias(b_down3, 1), w_conv3, bias(b_conv3, 1))
        return jnp.transpose(out, (2, 1, 0, 3))

    tile_spec = P('batch', 'row', 'col', None)
    return jax.shard_map(local, mesh=mesh, in_specs=(tile_spec,) + (P(),) * 12, out_specs=tile_spec, check_vma=False)
```

```python
import functools

import jax
import jax.numpy as jnp
from jax import lax
from jax.experimental import pallas as pl
from jax.experimental.pallas import tpu as pltpu
from jax.sharding import PartitionSpec as P

MESH = pl.DeviceIdType.MESH
F32 = jnp.float32
BF16 = jnp.bfloat16

N = 16
L = 128
C = 256
PIX = 640


def body(rows, cols, x_hbm, w_down1, b_down1, w_conv1_hbm, b_conv1, w_down2_hbm, b_down2, w_conv2_hbm, b_conv2, w_down3, b_down3,
         w_conv3, b_conv3, out_hbm, x_ref, w_conv1, w_down2, w_conv2, top, bot, tt, send_l, send_r, recv_l, recv_r, y1, z1, y2, z2, y3,
         wd1, wc1, wd2, wc2, wd3, wc3, biases, turn, out_ref, ssem, rsem, wsem, osem):
    r = lax.axis_index('row')
    c = lax.axis_index('col')
    has_up, has_dn = r > 0, r < rows - 1
    has_lf, has_rt = c > 0, c < cols - 1

    loads = [pltpu.make_async_copy(src, dst, wsem.at[k]) for k, (src, dst) in enumerate((
        (x_hbm, x_ref), (w_conv1_hbm, w_conv1), (w_down2_hbm, w_down2), (w_conv2_hbm, w_conv2), (w_down3, wd3), (w_conv3, wc3)))]
    for copy in loads:
        copy.start()

    neighbours = []
    for dr in (-1, 0, 1):
        for dc in (-1, 0, 1):
            if dr == 0 and dc == 0:
                continue
            there = None
            if dr:
                there = has_up if dr < 0 else has_dn
            if dc:
                side = has_lf if dc < 0 else has_rt
                there = side if there is None else jnp.logical_and(there, side)
            neighbours.append((dr, dc, there))

    def device(dr, dc):
        return {'row': r + dr, 'col': c + dc}

    barrier = pltpu.get_barrier_semaphore()
    for dr, dc, there in neighbours:
        @pl.when(there)
        def _():
            pl.semaphore_signal(barrier, inc=1, device_id=device(dr, dc), device_id_type=MESH)
    n_r = has_up.astype(jnp.int32) + has_dn.astype(jnp.int32)
    n_c = has_lf.astype(jnp.int32) + has_rt.astype(jnp.int32)
    pl.semaphore_wait(barrier, (n_r + 1) * (n_c + 1) - 1)

    def remote(src, dst, k, dr, dc):
        return pltpu.make_async_remote_copy(src_ref=src, dst_ref=dst, send_sem=ssem.at[k], recv_sem=rsem.at[k],
                                            device_id=device(dr, dc), device_id_type=MESH)

    to_dn = remote(x_ref.at[:, L - 8:L], top, 0, 1, 0)
    to_up = remote(x_ref.at[:, 0:8], bot, 1, -1, 0)
    loads[0].wait()

    @pl.when(has_dn)
    def _():
        to_dn.start()

    @pl.when(has_up)
    def _():
        to_up.start()

    def clear(ref, there, index):
        @pl.when(jnp.logical_not(there))
        def _():
            ref[index] = jnp.zeros_like(ref[index])

    every = slice(None)
    clear(top, has_up, (every,))
    clear(bot, has_dn, (every,))
    for copy in loads[1:4]:
        copy.wait()
    pack_weights(w_down1, w_conv1, w_down2, w_conv2, wd1, wc1, wd2, wc2)
    for k, b in enumerate((b_down1, b_conv1, b_down2, b_conv2, b_down3, b_conv3)):
        biases[k:k + 1, :] = jnp.concatenate([b[...]] * (C // b.shape[1]), axis=1)

    def put(cu, g, stack):
        t = jnp.transpose(stack.astype(F32))
        lanes = slice(g * L, g * L + L)
        tt[cu, 5:5 + L, lanes] = t
        send_l[cu, :, lanes] = t[0:8].astype(BF16)
        send_r[cu, :, lanes] = t[L - 8:L].astype(BF16)

    def inner(ch, _):
        for u in range(4):
            for g in (1, 2, 3):
                h0 = 32 * g + u - 5
                put(ch * 4 + u, g, jnp.concatenate([x_ref[ch, h0 + 4 * k] for k in range(8)], axis=0))
        return 0

    lax.fori_loop(0, 3, inner, 0)

    @pl.when(has_up)
    def _():
        to_up.wait_send()
        to_dn.wait_recv()

    @pl.when(has_dn)
    def _():
        to_dn.wait_send()
        to_up.wait_recv()

    def outer(ch, _):
        for u in range(4):
            for g in (0, 4):
                pieces = []
                for k in range(8):
                    h = 32 * g + u - 5 + 4 * k
                    if h < 0:
                        pieces.append(top[ch, h + 8])
                    elif h < L:
                        pieces.append(x_ref[ch, h])
                    elif h < L + 8:
                        pieces.append(bot[ch, h - L])
                    else:
                        pieces.append(jnp.zeros((N, L), BF16))
                put(ch * 4 + u, g, jnp.concatenate(pieces, axis=0))
        return 0

    lax.fori_loop(0, 3, outer, 0)

    to_lf = remote(send_l, recv_r, 2, 0, -1)
    to_rt = remote(send_r, recv_l, 3, 0, 1)

    @pl.when(has_lf)
    def _():
        to_lf.start()

    @pl.when(has_rt)
    def _():
        to_rt.start()

    def dots(pairs):
        acc = None
        for lhs, w in pairs:
            d = jnp.dot(lhs, w, preferred_element_type=F32)
            acc = d if acc is None else acc + d
        return acc

    def finish(acc, k, shape):
        return jnp.maximum(acc + biases[k:k + 1, :], 0.0).astype(BF16).reshape(shape)

    def loop(start, stop, unroll, step):
        assert (stop - start) % unroll == 0

        def run(t, _):
            for e in range(unroll):
                step(start + t * unroll + e)
            return 0

        lax.fori_loop(0, (stop - start) // unroll, run, 0)

    def down1(k):
        win = tt[:, pl.ds(8 * k if isinstance(k, int) else pl.multiple_of(8 * k, 8), N), :]
        for e in range(2):
            xt = jnp.transpose(win[:, 4 * e:4 * e + 8].reshape(96, PIX).astype(BF16))
            xb = jnp.concatenate([xt, jnp.zeros((PIX, L - 96), BF16)], axis=1)
            m = 34 * N
            lhs = jnp.concatenate([xb[0:m], xb[N:N + m]], axis=1)
            y1[2 * k + e] = finish(dots([(lhs, wd1[...])]), 0, (34, N, C))

    def conv1(b):
        pairs = [(y1[b + dw, dh:dh + 33].reshape(33 * N, C), wc1[dw, dh]) for dw in range(2) for dh in range(2)]
        z1[b] = finish(dots(pairs), 1, (33, N, C))

    loop(1, 16, 5, down1)
    clear(y1, has_up, (slice(2, 32), slice(0, 1)))
    clear(y1, has_dn, (slice(2, 32), slice(33, 34)))
    loop(2, 30, 7, conv1)

    @pl.when(has_lf)
    def _():
        to_lf.wait_send()
        to_rt.wait_recv()

    @pl.when(has_rt)
    def _():
        to_rt.wait_send()
        to_lf.wait_recv()

    clear(recv_l, has_lf, (every,))
    clear(recv_r, has_rt, (every,))
    tt[:, 0:5, :] = recv_l[...].astype(F32)[:, 3:8]
    tt[:, 5 + L:13 + L, :] = recv_r[...].astype(F32)
    down1(0)
    down1(N)
    for part in (slice(0, 2), slice(32, 34)):
        clear(y1, has_up, (part, slice(0, 1)))
        clear(y1, has_dn, (part, slice(33, 34)))
    clear(y1, has_lf, (slice(0, 1),))
    clear(y1, has_rt, (slice(33, 34),))
    for b in (0, 1, 30, 31, 32):
        conv1(b)
    clear(z1, has_up, (every, slice(0, 1), every, slice(0, L)))
    clear(z1, has_dn, (every, slice(32, 33), every, slice(L, C)))
    for half in (0, L):
        clear(z1, has_lf, (slice(0, 1), every, every, slice(half, half + 64)))
        clear(z1, has_rt, (slice(32, 33), every, every, slice(half + 64, half + L)))

    def edge(d, around, size, step):
        first, last = around, around + size
        if d == 0:
            return slice(first, last), slice(first, last)
        if d > 0:
            return slice(last - step, last), slice(first - step, first)
        return slice(first, first + step), slice(last, last + step)

    def start(copies):
        for copy, there, _ in copies:
            @pl.when(there)
            def _():
                copy.start()

    def finished(copies):
        for copy, there, back in copies:
            @pl.when(there)
            def _():
                copy.wait_send()
                back.wait_recv()

    def exchange(ref, k0, w_axis, h_axis, wanted):
        made = {}
        for k, (dr, dc, there) in enumerate(neighbours):
            if wanted(dr, dc):
                (ws, wd), (hs, hd) = edge(dc, *w_axis), edge(dr, *h_axis)
                made[k] = (remote(ref.at[ws, hs], ref.at[wd, hd], k0 + k, dr, dc), there)
        return [(copy, there, made[7 - k][0]) for k, (copy, there) in made.items()]

    def sideways(dr, dc):
        return dc != 0

    def upright(dr, dc):
        return dc == 0

    y2_cols = exchange(y2, 4, (1, N, 1), (2, 32, 2), sideways)
    y2_rows = [exchange(y2, k0, (w0, 8, 1), (2, 32, 2), upright) for k0, w0 in ((4, 1), (12, 9))]
    y3_cols = exchange(y3, 20, (1, N, 1), (1, N, 1), sideways)
    y3_rows = exchange(y3, 20, (1, N, 1), (1, N, 1), upright)

    def down2(p):
        pairs = [(z1[2 * p + dw, dh:dh + 32].reshape(32 * N, C), wd2[dw, dh]) for dw in range(3) for dh in range(2)]
        y2[p + 1, 2:34] = finish(dots(pairs), 2, (32, N, C))

    def conv2(q):
        pairs = [(y2[q + dw, dh:dh + 34].reshape(34 * N, C), wc2[dw, dh]) for dw in range(2) for dh in range(3)]
        z2[q] = finish(dots(pairs), 3, (34, N, C))

    for ref, step, last in ((y2, 2, 34), (y3, 1, 17)):
        clear(ref, has_up, (every, slice(0, step)))
        clear(ref, has_dn, (every, slice(last, last + step)))
        clear(ref, has_lf, (slice(0, 1),))
        clear(ref, has_rt, (slice(17, 18),))
    down2(0)
    down2(N - 1)
    start(y2_cols)
    loop(1, 8, 7, down2)
    start(y2_rows[0])
    loop(8, N - 1, 7, down2)
    start(y2_rows[1])
    finished(y2_rows[0])
    loop(1, 8, 7, conv2)
    finished(y2_rows[1])
    loop(8, N, 4, conv2)
    finished(y2_cols)
    conv2(0)
    conv2(N)
    clear(z2, has_up, (every, slice(0, 1)))
    clear(z2, has_dn, (every, slice(33, 34)))
    clear(z2, has_lf, (slice(0, 1), every, every, slice(0, L)))
    clear(z2, has_rt, (slice(N, N + 1), every, every, slice(L, C)))
    for copy in loads[4:]:
        copy.wait()

    def down3(k):
        pairs = []
        for dw in range(2):
            for dh in range(4):
                lhs = [z2[2 * k + e + dw, dh + 2 * i] for e in range(2) for i in range(N)]
                pairs.append((jnp.concatenate(lhs, axis=0), wd3[dh, 2 * dw:2 * dw + 2].reshape(C, C)))
        y3[pl.ds(2 * k + 1, 2), 1:17] = finish(dots(pairs), 4, (2, N, N, C))

    down3(0)
    down3(7)
    start(y3_cols)
    loop(1, 7, 3, down3)
    start(y3_rows)

    def conv3(pair, slot):
        pairs = []
        for dw in range(3):
            for dh in range(3):
                lhs = [y3[dw:dw + N, i + dh].reshape(C, C) for i in pair]
                pairs.append((jnp.concatenate(lhs, axis=0), wc3[dh, dw]))
        res = jnp.maximum(dots(pairs) + biases[5:6, :], 0.0)
        for e, i in enumerate(pair):
            at = 2 * slot + e
            for j in range(N):
                for half in range(2):
                    row = (N * e + j) * N
                    turn[at, half, pl.ds(j, N, stride=17), :] = res[row:row + N, half * L:half * L + L]
            for n in range(N):
                both = [turn[at, half, 17 * n:17 * n + N, :] for half in range(2)]
                out_ref[n, i] = jnp.concatenate(both, axis=1).astype(BF16)

    def put_out(i, size, k):
        return pltpu.make_async_copy(out_ref.at[:, pl.ds(i, size)], out_hbm.at[:, pl.ds(i, size)], osem.at[k])

    finished(y3_cols)

    def conv3_inner(t, _):
        for e in range(3):
            i = 6 * t + 2 * e + 1
            conv3((i, i + 1), e)
        put_out(6 * t + 1, 6, t).start()
        return 0

    lax.fori_loop(0, 2, conv3_inner, 0)
    finished(y3_rows)
    conv3((13, 14), 0)
    conv3((0, 15), 1)
    writes = [put_out(1, 6, 0), put_out(7, 6, 1), put_out(0, 1, 2), put_out(13, 3, 3)]
    for copy in writes[2:]:
        copy.start()
    for copy in writes:
        copy.wait()


def pack_weights(w_down1, w_conv1, w_down2, w_conv2, wd1, wc1, wd2, wc2):
    for dh in range(2):
        blocks = []
        for ch in range(3):
            for u in range(4):
                across = []
                for eh in range(2):
                    for ew in range(2):
                        kh = 4 * dh + u - 2 * eh
                        if 0 <= kh < 4:
                            down = [w_down1[kh, ch].astype(F32), jnp.zeros((4 - 2 * ew, 64), F32)]
                            across.append(jnp.concatenate(([jnp.zeros((2, 64), F32)] if ew else []) + down, axis=0))
                        else:
                            across.append(jnp.zeros((8, 64), F32))
                blocks.append(jnp.concatenate(across, axis=1))
        blocks.append(jnp.zeros((32, C), F32))
        wd1[L * dh:L * dh + L, :] = jnp.concatenate(blocks, axis=0).astype(BF16)
    for dw in range(2):
        for mw in range(2):
            for dh in range(2):
                for mh in range(2):
                    across = []
                    for eh in range(2):
                        for ew in range(2):
                            kh, kw = 2 * dh + mh - eh, 2 * dw + mw - ew
                            inside = 0 <= kh < 3 and 0 <= kw < 3
                            across.append(w_conv1[kh, kw] if inside else jnp.zeros((64, 64), BF16))
                    at = (2 * mh + mw) * 64
                    wc1[dw, dh, at:at + 64, :] = jnp.concatenate(across, axis=1)
    for dw in range(3):
        for mw in range(2):
            for dh in range(2):
                for mh in range(2):
                    at = (2 * mh + mw) * 64
                    for ew in range(2):
                        kw = 2 * dw + mw - 2 * ew
                        value = w_down2[2 * dh + mh, kw] if 0 <= kw < 4 else jnp.zeros((64, L), BF16)
                        wd2[dw, dh, at:at + 64, L * ew:L * ew + L] = value
    for dw in range(2):
        for mw in range(2):
            for kh in range(3):
                for ew in range(2):
                    kw = 2 * dw + mw - ew
                    value = w_conv2[kh, kw] if 0 <= kw < 3 else jnp.zeros((L, L), BF16)
                    wc2[dw, kh, L * mw:L * mw + L, L * ew:L * ew + L] = value


def solution(mesh):
    rows, cols = mesh.shape['row'], mesh.shape['col']

    def local(images, w_down1, b_down1, w_conv1, b_conv1, w_down2, b_down2, w_conv2, b_conv2, w_down3, b_down3, w_conv3, b_conv3):
        x = jnp.transpose(images, (3, 1, 0, 2))

        def row(b):
            return b.reshape(1, -1)

        def act(w, h):
            return pltpu.VMEM((w, h, N, C), BF16)

        vmem = pl.BlockSpec(memory_space=pltpu.VMEM)
        hbm = pl.BlockSpec(memory_space=pl.ANY)
        strip = pltpu.VMEM((12, 8, PIX), BF16)
        weight_in = [pltpu.VMEM(w.shape, BF16) for w in (w_conv1, w_down2, w_conv2)]
        weights = [pltpu.VMEM(shape, BF16) for shape in
                   ((C, C), (2, 2, C, C), (3, 2, C, C), (2, 3, C, C), w_down3.shape, w_conv3.shape)]
        dma = pltpu.SemaphoreType.DMA
        return pl.pallas_call(
            functools.partial(body, rows, cols),
            out_shape=jax.ShapeDtypeStruct((N, N, N, C), BF16),
            in_specs=[hbm, vmem, vmem] + [hbm, vmem] * 5,
            out_specs=hbm,
            scratch_shapes=[pltpu.VMEM((3, L, N, L), BF16)] + weight_in + [pltpu.VMEM((3, 8, N, L), BF16)] * 2
            + [pltpu.VMEM((12, 144, PIX), F32)] + [strip] * 4
            + [act(34, 34), act(33, 33), act(18, 36), act(17, 34), act(18, 18)] + weights
            + [pltpu.VMEM((8, C), F32), pltpu.VMEM((6, 2, 17 * N, L), F32), act(N, N), dma((28,)), dma((28,)), dma((6,)), dma((4,))],
            compiler_params=pltpu.CompilerParams(collective_id=0, has_side_effects=True, vmem_limit_bytes=66_000_000),
            name='encoder',
        )(x, jnp.transpose(w_down1, (0, 2, 1, 3)), row(b_down1), w_conv1, row(b_conv1), w_down2, row(b_down2), w_conv2, row(b_conv2),
          w_down3, row(b_down3), w_conv3, row(b_conv3))

    tile_spec = P('batch', 'row', 'col', None)
    return jax.shard_map(local, mesh=mesh, in_specs=(tile_spec,) + (P(),) * 12, out_specs=tile_spec, check_vma=False)
```

```python
import functools

import jax
import jax.numpy as jnp
from jax import lax
from jax.experimental import pallas as pl
from jax.experimental.pallas import tpu as pltpu
from jax.sharding import PartitionSpec as P

MESH = pl.DeviceIdType.MESH
F32 = jnp.float32
BF16 = jnp.bfloat16

N = 16
L = 128
C = 256
PIX = 640


def body(rows, cols, x_hbm, w_down1, b_down1, w_conv1_hbm, b_conv1, w_down2_hbm, b_down2, w_conv2_hbm, b_conv2, w_down3, b_down3,
         w_conv3, b_conv3, out_hbm, x_ref, w_conv1, w_down2, w_conv2, top, bot, xs, tt, send_l, send_r, recv_l, recv_r, y1, z1, y2, z2, y3,
         wd1, wc1, wd2, wc2, wd3, wc3, biases, turn, out_ref, ssem, rsem, wsem, osem):
    r = lax.axis_index('row')
    c = lax.axis_index('col')
    has_up, has_dn = r > 0, r < rows - 1
    has_lf, has_rt = c > 0, c < cols - 1

    loads = [pltpu.make_async_copy(src, dst, wsem.at[k]) for k, (src, dst) in enumerate((
        (x_hbm, x_ref), (w_conv1_hbm, w_conv1), (w_down2_hbm, w_down2), (w_conv2_hbm, w_conv2), (w_down3, wd3), (w_conv3, wc3)))]
    for copy in loads:
        copy.start()

    neighbours = []
    for dr in (-1, 0, 1):
        for dc in (-1, 0, 1):
            if dr == 0 and dc == 0:
                continue
            there = None
            if dr:
                there = has_up if dr < 0 else has_dn
            if dc:
                side = has_lf if dc < 0 else has_rt
                there = side if there is None else jnp.logical_and(there, side)
            neighbours.append((dr, dc, there))

    def device(dr, dc):
        return {'row': r + dr, 'col': c + dc}

    barrier = pltpu.get_barrier_semaphore()
    for dr, dc, there in neighbours:
        @pl.when(there)
        def _():
            pl.semaphore_signal(barrier, inc=1, device_id=device(dr, dc), device_id_type=MESH)
    n_r = has_up.astype(jnp.int32) + has_dn.astype(jnp.int32)
    n_c = has_lf.astype(jnp.int32) + has_rt.astype(jnp.int32)
    pl.semaphore_wait(barrier, (n_r + 1) * (n_c + 1) - 1)

    def remote(src, dst, k, dr, dc):
        return pltpu.make_async_remote_copy(src_ref=src, dst_ref=dst, send_sem=ssem.at[k], recv_sem=rsem.at[k],
                                            device_id=device(dr, dc), device_id_type=MESH)

    to_dn = remote(x_ref.at[:, :, L - 8:L], top, 0, 1, 0)
    to_up = remote(x_ref.at[:, :, 0:8], bot, 1, -1, 0)
    loads[0].wait()

    @pl.when(has_dn)
    def _():
        to_dn.start()

    @pl.when(has_up)
    def _():
        to_up.start()

    def clear(ref, there, index):
        @pl.when(jnp.logical_not(there))
        def _():
            ref[index] = jnp.zeros_like(ref[index])

    every = slice(None)
    clear(top, has_up, (every,))
    clear(bot, has_dn, (every,))
    for copy in loads[1:4]:
        copy.wait()
    pack_weights(w_down1, w_conv1, w_down2, w_conv2, wd1, wc1, wd2, wc2)
    for k, b in enumerate((b_down1, b_conv1, b_down2, b_conv2, b_down3, b_conv3)):
        biases[k:k + 1, :] = jnp.concatenate([b[...]] * (C // b.shape[1]), axis=1)

    def gather(ch, src, h, size):
        for n in range(N):
            xs[ch, pl.ds(17 * (h + 8) + n, size, stride=17), :] = src[n, ch].astype(F32)

    def put(ch, g):
        for u in range(4):
            pieces = []
            for k in range(8):
                at = 17 * (32 * g + u + 3 + 4 * k)
                pieces.append(xs[ch, at:at + N, :] if at < 17 * (L + N) else jnp.zeros((N, L), F32))
            t = jnp.transpose(jnp.concatenate(pieces, axis=0))
            cu = ch * 4 + u
            lanes = slice(g * L, g * L + L)
            tt[cu, 5:5 + L, lanes] = t
            send_l[cu, :, lanes] = t[0:8].astype(BF16)
            send_r[cu, :, lanes] = t[L - 8:L].astype(BF16)

    def inner(ch, _):
        gather(ch, x_ref, 0, L)
        for g in (1, 2, 3):
            put(ch, g)
        return 0

    lax.fori_loop(0, 3, inner, 0)

    @pl.when(has_up)
    def _():
        to_up.wait_send()
        to_dn.wait_recv()

    @pl.when(has_dn)
    def _():
        to_dn.wait_send()
        to_up.wait_recv()

    def outer(ch, _):
        gather(ch, top, -8, 8)
        gather(ch, bot, L, 8)
        for g in (0, 4):
            put(ch, g)
        return 0

    lax.fori_loop(0, 3, outer, 0)

    to_lf = remote(send_l, recv_r, 2, 0, -1)
    to_rt = remote(send_r, recv_l, 3, 0, 1)

    @pl.when(has_lf)
    def _():
        to_lf.start()

    @pl.when(has_rt)
    def _():
        to_rt.start()

    def dots(pairs):
        acc = None
        for lhs, w in pairs:
            d = jnp.dot(lhs, w, preferred_element_type=F32)
            acc = d if acc is None else acc + d
        return acc

    def finish(acc, k, shape):
        return jnp.maximum(acc + biases[k:k + 1, :], 0.0).astype(BF16).reshape(shape)

    def loop(start, stop, unroll, step):
        assert (stop - start) % unroll == 0

        def run(t, _):
            for e in range(unroll):
                step(start + t * unroll + e)
            return 0

        lax.fori_loop(0, (stop - start) // unroll, run, 0)

    def down1(k):
        win = tt[:, pl.ds(8 * k if isinstance(k, int) else pl.multiple_of(8 * k, 8), N), :]
        for e in range(2):
            xt = jnp.transpose(win[:, 4 * e:4 * e + 8].reshape(96, PIX).astype(BF16))
            xb = jnp.concatenate([xt, jnp.zeros((PIX, L - 96), BF16)], axis=1)
            m = 34 * N
            lhs = jnp.concatenate([xb[0:m], xb[N:N + m]], axis=1)
            y1[2 * k + e] = finish(dots([(lhs, wd1[...])]), 0, (34, N, C))

    def conv1(b):
        pairs = [(y1[b + dw, dh:dh + 33].reshape(33 * N, C), wc1[dw, dh]) for dw in range(2) for dh in range(2)]
        z1[b] = finish(dots(pairs), 1, (33, N, C))

    loop(1, 16, 5, down1)
    clear(y1, has_up, (slice(2, 32), slice(0, 1)))
    clear(y1, has_dn, (slice(2, 32), slice(33, 34)))
    loop(2, 30, 14, conv1)

    @pl.when(has_lf)
    def _():
        to_lf.wait_send()
        to_rt.wait_recv()

    @pl.when(has_rt)
    def _():
        to_rt.wait_send()
        to_lf.wait_recv()

    clear(recv_l, has_lf, (every,))
    clear(recv_r, has_rt, (every,))
    tt[:, 0:5, :] = recv_l[...].astype(F32)[:, 3:8]
    tt[:, 5 + L:13 + L, :] = recv_r[...].astype(F32)
    down1(0)
    down1(N)
    for part in (slice(0, 2), slice(32, 34)):
        clear(y1, has_up, (part, slice(0, 1)))
        clear(y1, has_dn, (part, slice(33, 34)))
    clear(y1, has_lf, (slice(0, 1),))
    clear(y1, has_rt, (slice(33, 34),))
    for b in (0, 1, 30, 31, 32):
        conv1(b)
    clear(z1, has_up, (every, slice(0, 1), every, slice(0, L)))
    clear(z1, has_dn, (every, slice(32, 33), every, slice(L, C)))
    for half in (0, L):
        clear(z1, has_lf, (slice(0, 1), every, every, slice(half, half + 64)))
        clear(z1, has_rt, (slice(32, 33), every, every, slice(half + 64, half + L)))

    def edge(d, around, size, step):
        first, last = around, around + size
        if d == 0:
            return slice(first, last), slice(first, last)
        if d > 0:
            return slice(last - step, last), slice(first - step, first)
        return slice(first, first + step), slice(last, last + step)

    def start(copies):
        for copy, there, _ in copies:
            @pl.when(there)
            def _():
                copy.start()

    def finished(copies):
        for copy, there, back in copies:
            @pl.when(there)
            def _():
                copy.wait_send()
                back.wait_recv()

    def exchange(ref, k0, w_axis, h_axis, wanted):
        made = {}
        for k, (dr, dc, there) in enumerate(neighbours):
            if wanted(dr, dc):
                (ws, wd), (hs, hd) = edge(dc, *w_axis), edge(dr, *h_axis)
                made[k] = (remote(ref.at[ws, hs], ref.at[wd, hd], k0 + k, dr, dc), there)
        return [(copy, there, made[7 - k][0]) for k, (copy, there) in made.items()]

    def sideways(dr, dc):
        return dc != 0

    def upright(dr, dc):
        return dc == 0

    y2_cols = exchange(y2, 4, (1, N, 1), (2, 32, 2), sideways)
    y2_rows = [exchange(y2, k0, (w0, 8, 1), (2, 32, 2), upright) for k0, w0 in ((4, 1), (12, 9))]
    y3_cols = exchange(y3, 20, (1, N, 1), (1, N, 1), sideways)
    y3_rows = exchange(y3, 20, (1, N, 1), (1, N, 1), upright)

    def down2(p):
        pairs = [(z1[2 * p + dw, dh:dh + 32].reshape(32 * N, C), wd2[dw, dh]) for dw in range(3) for dh in range(2)]
        y2[p + 1, 2:34] = finish(dots(pairs), 2, (32, N, C))

    def conv2(q):
        pairs = [(y2[q + dw, dh:dh + 34].reshape(34 * N, C), wc2[dw, dh]) for dw in range(2) for dh in range(3)]
        z2[q] = finish(dots(pairs), 3, (34, N, C))

    for ref, step, last in ((y2, 2, 34), (y3, 1, 17)):
        clear(ref, has_up, (every, slice(0, step)))
        clear(ref, has_dn, (every, slice(last, last + step)))
        clear(ref, has_lf, (slice(0, 1),))
        clear(ref, has_rt, (slice(17, 18),))
    down2(0)
    down2(N - 1)
    start(y2_cols)
    loop(1, 8, 7, down2)
    start(y2_rows[0])
    loop(8, N - 1, 7, down2)
    start(y2_rows[1])
    finished(y2_rows[0])
    loop(1, 8, 7, conv2)
    finished(y2_rows[1])
    loop(8, N, 8, conv2)
    finished(y2_cols)
    conv2(0)
    conv2(N)
    clear(z2, has_up, (every, slice(0, 1)))
    clear(z2, has_dn, (every, slice(33, 34)))
    clear(z2, has_lf, (slice(0, 1), every, every, slice(0, L)))
    clear(z2, has_rt, (slice(N, N + 1), every, every, slice(L, C)))
    for copy in loads[4:]:
        copy.wait()

    def down3(k):
        pairs = []
        for dw in range(2):
            for dh in range(4):
                lhs = [z2[2 * k + e + dw, dh + 2 * i] for e in range(2) for i in range(N)]
                pairs.append((jnp.concatenate(lhs, axis=0), wd3[dh, 2 * dw:2 * dw + 2].reshape(C, C)))
        y3[pl.ds(2 * k + 1, 2), 1:17] = finish(dots(pairs), 4, (2, N, N, C))

    down3(0)
    down3(7)
    start(y3_cols)
    loop(1, 7, 6, down3)
    start(y3_rows)

    def conv3(pair, slot):
        pairs = []
        for dw in range(3):
            for dh in range(3):
                lhs = [y3[dw:dw + N, i + dh].reshape(C, C) for i in pair]
                pairs.append((jnp.concatenate(lhs, axis=0), wc3[dh, dw]))
        res = dots(pairs) + biases[5:6, :]
        for e, i in enumerate(pair):
            at = 2 * slot + e
            for j in range(N):
                for half in range(2):
                    row = (N * e + j) * N
                    turn[at, half, pl.ds(j, N, stride=17), :] = res[row:row + N, half * L:half * L + L]
            for n in range(N):
                both = [turn[at, half, 17 * n:17 * n + N, :] for half in range(2)]
                out_ref[n, i] = jnp.concatenate(both, axis=1).astype(BF16)

    def put_out(i, size, k):
        return pltpu.make_async_copy(out_ref.at[:, pl.ds(i, size)], out_hbm.at[:, pl.ds(i, size)], osem.at[k])

    finished(y3_cols)

    def conv3_inner(t, _):
        for e in range(3):
            i = 6 * t + 2 * e + 1
            conv3((i, i + 1), e)
        put_out(6 * t + 1, 6, t).start()
        return 0

    lax.fori_loop(0, 2, conv3_inner, 0)
    finished(y3_rows)
    conv3((13, 14), 0)
    conv3((0, 15), 1)
    writes = [put_out(1, 6, 0), put_out(7, 6, 1), put_out(0, 1, 2), put_out(13, 3, 3)]
    for copy in writes[2:]:
        copy.start()
    for copy in writes:
        copy.wait()


def pack_weights(w_down1, w_conv1, w_down2, w_conv2, wd1, wc1, wd2, wc2):
    for dh in range(2):
        blocks = []
        for ch in range(3):
            for u in range(4):
                across = []
                for eh in range(2):
                    for ew in range(2):
                        kh = 4 * dh + u - 2 * eh
                        if 0 <= kh < 4:
                            down = [w_down1[kh, ch].astype(F32), jnp.zeros((4 - 2 * ew, 64), F32)]
                            across.append(jnp.concatenate(([jnp.zeros((2, 64), F32)] if ew else []) + down, axis=0))
                        else:
                            across.append(jnp.zeros((8, 64), F32))
                blocks.append(jnp.concatenate(across, axis=1))
        blocks.append(jnp.zeros((32, C), F32))
        wd1[L * dh:L * dh + L, :] = jnp.concatenate(blocks, axis=0).astype(BF16)
    for dw in range(2):
        for mw in range(2):
            for dh in range(2):
                for mh in range(2):
                    across = []
                    for eh in range(2):
                        for ew in range(2):
                            kh, kw = 2 * dh + mh - eh, 2 * dw + mw - ew
                            inside = 0 <= kh < 3 and 0 <= kw < 3
                            across.append(w_conv1[kh, kw] if inside else jnp.zeros((64, 64), BF16))
                    at = (2 * mh + mw) * 64
                    wc1[dw, dh, at:at + 64, :] = jnp.concatenate(across, axis=1)
    for dw in range(3):
        for mw in range(2):
            for dh in range(2):
                for mh in range(2):
                    at = (2 * mh + mw) * 64
                    for ew in range(2):
                        kw = 2 * dw + mw - 2 * ew
                        value = w_down2[2 * dh + mh, kw] if 0 <= kw < 4 else jnp.zeros((64, L), BF16)
                        wd2[dw, dh, at:at + 64, L * ew:L * ew + L] = value
    for dw in range(2):
        for mw in range(2):
            for kh in range(3):
                for ew in range(2):
                    kw = 2 * dw + mw - ew
                    value = w_conv2[kh, kw] if 0 <= kw < 3 else jnp.zeros((L, L), BF16)
                    wc2[dw, kh, L * mw:L * mw + L, L * ew:L * ew + L] = value


def solution(mesh):
    rows, cols = mesh.shape['row'], mesh.shape['col']

    def local(images, w_down1, b_down1, w_conv1, b_conv1, w_down2, b_down2, w_conv2, b_conv2, w_down3, b_down3, w_conv3, b_conv3):
        x = jnp.transpose(images, (0, 3, 1, 2))

        def row(b):
            return b.reshape(1, -1)

        def act(w, h):
            return pltpu.VMEM((w, h, N, C), BF16)

        vmem = pl.BlockSpec(memory_space=pltpu.VMEM)
        hbm = pl.BlockSpec(memory_space=pl.ANY)
        strip = pltpu.VMEM((12, 8, PIX), BF16)
        weight_in = [pltpu.VMEM(w.shape, BF16) for w in (w_conv1, w_down2, w_conv2)]
        weights = [pltpu.VMEM(shape, BF16) for shape in
                   ((C, C), (2, 2, C, C), (3, 2, C, C), (2, 3, C, C), w_down3.shape, w_conv3.shape)]
        dma = pltpu.SemaphoreType.DMA
        out = pl.pallas_call(
            functools.partial(body, rows, cols),
            out_shape=jax.ShapeDtypeStruct((N, N, N, C), BF16),
            in_specs=[hbm, vmem, vmem] + [hbm, vmem] * 5,
            out_specs=hbm,
            scratch_shapes=[pltpu.VMEM((N, 3, L, L), BF16)] + weight_in + [pltpu.VMEM((N, 3, 8, L), BF16)] * 2
            + [pltpu.VMEM((3, 17 * (L + N), L), F32), pltpu.VMEM((12, 144, PIX), F32)] + [strip] * 4
            + [act(34, 34), act(33, 33), act(18, 36), act(17, 34), act(18, 18)] + weights
            + [pltpu.VMEM((8, C), F32), pltpu.VMEM((6, 2, 17 * N, L), F32), act(N, N), dma((28,)), dma((28,)), dma((6,)), dma((4,))],
            compiler_params=pltpu.CompilerParams(collective_id=0, has_side_effects=True, vmem_limit_bytes=66_000_000),
            name='encoder',
        )(x, jnp.transpose(w_down1, (0, 2, 1, 3)), row(b_down1), w_conv1, row(b_conv1), w_down2, row(b_down2), w_conv2, row(b_conv2),
          w_down3, row(b_down3), w_conv3, row(b_conv3))
        return jnp.maximum(out, jnp.zeros_like(out))

    tile_spec = P('batch', 'row', 'col', None)
    return jax.shard_map(local, mesh=mesh, in_specs=(tile_spec,) + (P(),) * 12, out_specs=tile_spec, check_vma=False)
```

```python
import functools

import jax
import jax.numpy as jnp
from jax import lax
from jax.experimental import pallas as pl
from jax.experimental.pallas import tpu as pltpu
from jax.sharding import PartitionSpec as P

MESH = pl.DeviceIdType.MESH
F32 = jnp.float32
BF16 = jnp.bfloat16

N = 16
L = 128
C = 256
PIX = 640


def body(rows, cols, x_hbm, w_down1, b_down1, w_conv1_hbm, b_conv1, w_down2_hbm, b_down2, w_conv2_hbm, b_conv2, w_down3, b_down3,
         w_conv3, b_conv3, out_hbm, x_ref, w_conv1, w_down2, w_conv2, top, bot, xs, tt, send_l, send_r, recv_l, recv_r, y1, z1, y2, z2, y3,
         wd1, wc1, wd2, wc2, wd3, wc3, biases, turn, out_ref, ssem, rsem, wsem, osem):
    r = lax.axis_index('row')
    c = lax.axis_index('col')
    has_up, has_dn = r > 0, r < rows - 1
    has_lf, has_rt = c > 0, c < cols - 1

    loads = [pltpu.make_async_copy(src, dst, wsem.at[k]) for k, (src, dst) in enumerate((
        (x_hbm, x_ref), (w_conv1_hbm, w_conv1), (w_down2_hbm, w_down2), (w_conv2_hbm, w_conv2), (w_down3, wd3), (w_conv3, wc3)))]
    for copy in loads:
        copy.start()

    neighbours = []
    for dr in (-1, 0, 1):
        for dc in (-1, 0, 1):
            if dr == 0 and dc == 0:
                continue
            there = None
            if dr:
                there = has_up if dr < 0 else has_dn
            if dc:
                side = has_lf if dc < 0 else has_rt
                there = side if there is None else jnp.logical_and(there, side)
            neighbours.append((dr, dc, there))

    def device(dr, dc):
        return {'row': r + dr, 'col': c + dc}

    barrier = pltpu.get_barrier_semaphore()
    for dr, dc, there in neighbours:
        if dr and dc:
            continue

        @pl.when(there)
        def _():
            pl.semaphore_signal(barrier, inc=1, device_id=device(dr, dc), device_id_type=MESH)
    pl.semaphore_wait(barrier, sum(t.astype(jnp.int32) for t in (has_up, has_dn, has_lf, has_rt)))

    def remote(src, dst, k, dr, dc):
        return pltpu.make_async_remote_copy(src_ref=src, dst_ref=dst, send_sem=ssem.at[k], recv_sem=rsem.at[k],
                                            device_id=device(dr, dc), device_id_type=MESH)

    to_dn = remote(x_ref.at[:, :, L - 8:L], top, 0, 1, 0)
    to_up = remote(x_ref.at[:, :, 0:8], bot, 1, -1, 0)
    loads[0].wait()

    @pl.when(has_dn)
    def _():
        to_dn.start()

    @pl.when(has_up)
    def _():
        to_up.start()

    def clear(ref, there, index):
        @pl.when(jnp.logical_not(there))
        def _():
            ref[index] = jnp.zeros_like(ref[index])

    every = slice(None)
    clear(top, has_up, (every,))
    clear(bot, has_dn, (every,))
    for copy in loads[1:4]:
        copy.wait()
    pack_weights(w_down1, w_conv1, w_down2, w_conv2, wd1, wc1, wd2, wc2)
    for k, b in enumerate((b_down1, b_conv1, b_down2, b_conv2, b_down3, b_conv3)):
        biases[k:k + 1, :] = jnp.concatenate([b[...]] * (C // b.shape[1]), axis=1)

    def gather(ch, src, h, size):
        for n in range(N):
            xs[ch, pl.ds(17 * (h + 8) + n, size, stride=17), :] = src[n, ch].astype(F32)

    def put(ch, g):
        for u in range(4):
            pieces = []
            for k in range(8):
                at = 17 * (32 * g + u + 3 + 4 * k)
                pieces.append(xs[ch, at:at + N, :] if at < 17 * (L + N) else jnp.zeros((N, L), F32))
            t = jnp.transpose(jnp.concatenate(pieces, axis=0))
            cu = ch * 4 + u
            lanes = slice(g * L, g * L + L)
            tt[cu, 5:5 + L, lanes] = t
            send_l[cu, :, lanes] = t[0:8].astype(BF16)
            send_r[cu, :, lanes] = t[L - 8:L].astype(BF16)

    def inner(ch, _):
        gather(ch, x_ref, 0, L)
        for g in (1, 2, 3):
            put(ch, g)
        return 0

    lax.fori_loop(0, 3, inner, 0)

    @pl.when(has_up)
    def _():
        to_up.wait_send()
        to_dn.wait_recv()

    @pl.when(has_dn)
    def _():
        to_dn.wait_send()
        to_up.wait_recv()

    def outer(ch, _):
        gather(ch, top, -8, 8)
        gather(ch, bot, L, 8)
        for g in (0, 4):
            put(ch, g)
        return 0

    lax.fori_loop(0, 3, outer, 0)

    to_lf = remote(send_l, recv_r, 2, 0, -1)
    to_rt = remote(send_r, recv_l, 3, 0, 1)

    @pl.when(has_lf)
    def _():
        to_lf.start()

    @pl.when(has_rt)
    def _():
        to_rt.start()

    def dots(pairs):
        acc = None
        for lhs, w in pairs:
            d = jnp.dot(lhs, w, preferred_element_type=F32)
            acc = d if acc is None else acc + d
        return acc

    def finish(acc, k, shape):
        return jnp.maximum(acc + biases[k:k + 1, :], 0.0).astype(BF16).reshape(shape)

    def loop(start, stop, unroll, step):
        assert (stop - start) % unroll == 0

        def run(t, _):
            for e in range(unroll):
                step(start + t * unroll + e)
            return 0

        lax.fori_loop(0, (stop - start) // unroll, run, 0)

    def down1(k):
        win = tt[:, pl.ds(8 * k if isinstance(k, int) else pl.multiple_of(8 * k, 8), N), :]
        for e in range(2):
            xt = jnp.transpose(win[:, 4 * e:4 * e + 8].reshape(96, PIX).astype(BF16))
            xb = jnp.concatenate([xt, jnp.zeros((PIX, L - 96), BF16)], axis=1)
            m = 34 * N
            lhs = jnp.concatenate([xb[0:m], xb[N:N + m]], axis=1)
            y1[2 * k + e] = finish(dots([(lhs, wd1[...])]), 0, (34, N, C))

    def conv1(b):
        pairs = [(y1[b + dw, dh:dh + 33].reshape(33 * N, C), wc1[dw, dh]) for dw in range(2) for dh in range(2)]
        z1[b] = finish(dots(pairs), 1, (33, N, C))

    loop(1, 16, 5, down1)
    clear(y1, has_up, (slice(2, 32), slice(0, 1)))
    clear(y1, has_dn, (slice(2, 32), slice(33, 34)))
    loop(2, 30, 14, conv1)

    @pl.when(has_lf)
    def _():
        to_lf.wait_send()
        to_rt.wait_recv()

    @pl.when(has_rt)
    def _():
        to_rt.wait_send()
        to_lf.wait_recv()

    clear(recv_l, has_lf, (every,))
    clear(recv_r, has_rt, (every,))
    tt[:, 0:5, :] = recv_l[...].astype(F32)[:, 3:8]
    tt[:, 5 + L:13 + L, :] = recv_r[...].astype(F32)
    down1(0)
    down1(N)
    for part in (slice(0, 2), slice(32, 34)):
        clear(y1, has_up, (part, slice(0, 1)))
        clear(y1, has_dn, (part, slice(33, 34)))
    clear(y1, has_lf, (slice(0, 1),))
    clear(y1, has_rt, (slice(33, 34),))
    for b in (0, 1, 30, 31, 32):
        conv1(b)
    clear(z1, has_up, (every, slice(0, 1), every, slice(0, L)))
    clear(z1, has_dn, (every, slice(32, 33), every, slice(L, C)))
    for half in (0, L):
        clear(z1, has_lf, (slice(0, 1), every, every, slice(half, half + 64)))
        clear(z1, has_rt, (slice(32, 33), every, every, slice(half + 64, half + L)))

    def edge(d, around, size, step):
        first, last = around, around + size
        if d == 0:
            return slice(first, last), slice(first, last)
        if d > 0:
            return slice(last - step, last), slice(first - step, first)
        return slice(first, first + step), slice(last, last + step)

    def start(copies):
        for copy, there, _ in copies:
            @pl.when(there)
            def _():
                copy.start()

    def finished(copies):
        for copy, there, back in copies:
            @pl.when(there)
            def _():
                copy.wait_send()
                back.wait_recv()

    def exchange(ref, k0, w_axis, h_axis, wanted):
        made = {}
        for k, (dr, dc, there) in enumerate(neighbours):
            if wanted(dr, dc):
                (ws, wd), (hs, hd) = edge(dc, *w_axis), edge(dr, *h_axis)
                made[k] = (remote(ref.at[ws, hs], ref.at[wd, hd], k0 + k, dr, dc), there)
        return [(copy, there, made[7 - k][0]) for k, (copy, there) in made.items()]

    def sideways(dr, dc):
        return dc != 0

    def upright(dr, dc):
        return dc == 0

    y2_cols = exchange(y2, 4, (1, N, 1), (2, 32, 2), sideways)
    y2_rows = [exchange(y2, k0, (w0, 8, 1), (2, 32, 2), upright) for k0, w0 in ((4, 1), (12, 9))]
    y3_cols = exchange(y3, 20, (1, N, 1), (1, N, 1), sideways)
    y3_rows = exchange(y3, 20, (1, N, 1), (1, N, 1), upright)

    def down2(p):
        pairs = [(z1[2 * p + dw, dh:dh + 32].reshape(32 * N, C), wd2[dw, dh]) for dw in range(3) for dh in range(2)]
        y2[p + 1, 2:34] = finish(dots(pairs), 2, (32, N, C))

    def conv2(q):
        pairs = [(y2[q + dw, dh:dh + 34].reshape(34 * N, C), wc2[dw, dh]) for dw in range(2) for dh in range(3)]
        z2[q] = finish(dots(pairs), 3, (34, N, C))

    def conv2_inner(q):
        pairs = [(y2[q + dw, dh + 2:dh + 32].reshape(30 * N, C), wc2[dw, dh]) for dw in range(2) for dh in range(3)]
        z2[q, 2:32] = finish(dots(pairs), 3, (30, N, C))

    def conv2_rest(first, last):
        pairs = []
        for dw in range(2):
            for dh in range(3):
                lhs = [y2[q + dw, h + dh:h + dh + 2].reshape(2 * N, C) for q in range(first, last) for h in (0, 32)]
                pairs.append((jnp.concatenate(lhs, axis=0), wc2[dw, dh]))
        res = finish(dots(pairs), 3, (last - first, 4, N, C))
        z2[first:last, 0:2] = res[:, 0:2]
        z2[first:last, 32:34] = res[:, 2:4]

    for ref, step, last in ((y2, 2, 34), (y3, 1, 17)):
        clear(ref, has_up, (every, slice(0, step)))
        clear(ref, has_dn, (every, slice(last, last + step)))
        clear(ref, has_lf, (slice(0, 1),))
        clear(ref, has_rt, (slice(17, 18),))
    down2(0)
    down2(N - 1)
    start(y2_cols)
    loop(1, 8, 7, down2)
    start(y2_rows[0])
    loop(8, N - 1, 7, down2)
    start(y2_rows[1])
    for q in range(3, 12):
        conv2_inner(q)
    for copies in (*y2_rows, y2_cols):
        finished(copies)
    outer_q = (slice(0, 3), slice(14, 17))
    for part in outer_q:
        for q in range(part.start, part.stop):
            conv2(q)
    for part in outer_q:
        clear(z2, has_up, (part, slice(0, 1)))
        clear(z2, has_dn, (part, slice(33, 34)))
    clear(z2, has_lf, (slice(0, 1), every, every, slice(0, L)))
    clear(z2, has_rt, (slice(N, N + 1), every, every, slice(L, C)))
    for copy in loads[4:]:
        copy.wait()

    def down3(k):
        pairs = []
        for dw in range(2):
            for dh in range(4):
                lhs = [z2[2 * k + e + dw, dh + 2 * i] for e in range(2) for i in range(N)]
                pairs.append((jnp.concatenate(lhs, axis=0), wd3[dh, 2 * dw:2 * dw + 2].reshape(C, C)))
        y3[pl.ds(2 * k + 1, 2), 1:17] = finish(dots(pairs), 4, (2, N, N, C))

    down3(0)
    down3(7)
    start(y3_cols)
    conv2_inner(12)
    conv2_inner(13)
    conv2_rest(3, 14)
    clear(z2, has_up, (slice(3, 14), slice(0, 1)))
    clear(z2, has_dn, (slice(3, 14), slice(33, 34)))
    for k in range(1, 7):
        down3(k)
    start(y3_rows)

    def conv3(pair, slot):
        pairs = []
        for dw in range(3):
            for dh in range(3):
                lhs = [y3[dw:dw + N, i + dh].reshape(C, C) for i in pair]
                pairs.append((jnp.concatenate(lhs, axis=0), wc3[dh, dw]))
        res = jnp.maximum(dots(pairs) + biases[5:6, :], 0.0)
        for e, i in enumerate(pair):
            at = 2 * slot + e
            for j in range(N):
                for half in range(2):
                    row = (N * e + j) * N
                    turn[at, half, pl.ds(j, N, stride=17), :] = res[row:row + N, half * L:half * L + L]
            for n in range(N):
                both = [turn[at, half, 17 * n:17 * n + N, :] for half in range(2)]
                out_ref[n, i] = jnp.concatenate(both, axis=1).astype(BF16)

    def put_out(i, size, k):
        return pltpu.make_async_copy(out_ref.at[:, pl.ds(i, size)], out_hbm.at[:, pl.ds(i, size)], osem.at[k])

    finished(y3_cols)

    def conv3_inner(t, _):
        for e in range(3):
            i = 6 * t + 2 * e + 1
            conv3((i, i + 1), e)
        put_out(6 * t + 1, 6, t).start()
        return 0

    lax.fori_loop(0, 2, conv3_inner, 0)
    finished(y3_rows)
    conv3((13, 14), 0)
    conv3((0, 15), 1)
    writes = [put_out(1, 6, 0), put_out(7, 6, 1), put_out(0, 1, 2), put_out(13, 3, 3)]
    for copy in writes[2:]:
        copy.start()
    for copy in writes:
        copy.wait()


def hand_on(src, dst, held, isem, osem):
    parts = [pl.ds(2 * k, 2) for k in range(8)]
    reads = [pltpu.make_async_copy(src.at[p], held.at[p], isem.at[k]) for k, p in enumerate(parts)]
    writes = [pltpu.make_async_copy(held.at[p], dst.at[p], osem.at[k]) for k, p in enumerate(parts)]
    for copy in reads:
        copy.start()
    for read, write in zip(reads, writes):
        read.wait()
        write.start()
    for copy in writes:
        copy.wait()


def pack_weights(w_down1, w_conv1, w_down2, w_conv2, wd1, wc1, wd2, wc2):
    for dh in range(2):
        blocks = []
        for ch in range(3):
            for u in range(4):
                across = []
                for eh in range(2):
                    for ew in range(2):
                        kh = 4 * dh + u - 2 * eh
                        if 0 <= kh < 4:
                            down = [w_down1[kh, ch].astype(F32), jnp.zeros((4 - 2 * ew, 64), F32)]
                            across.append(jnp.concatenate(([jnp.zeros((2, 64), F32)] if ew else []) + down, axis=0))
                        else:
                            across.append(jnp.zeros((8, 64), F32))
                blocks.append(jnp.concatenate(across, axis=1))
        blocks.append(jnp.zeros((32, C), F32))
        wd1[L * dh:L * dh + L, :] = jnp.concatenate(blocks, axis=0).astype(BF16)
    for dw in range(2):
        for mw in range(2):
            for dh in range(2):
                for mh in range(2):
                    across = []
                    for eh in range(2):
                        for ew in range(2):
                            kh, kw = 2 * dh + mh - eh, 2 * dw + mw - ew
                            inside = 0 <= kh < 3 and 0 <= kw < 3
                            across.append(w_conv1[kh, kw] if inside else jnp.zeros((64, 64), BF16))
                    at = (2 * mh + mw) * 64
                    wc1[dw, dh, at:at + 64, :] = jnp.concatenate(across, axis=1)
    for dw in range(3):
        for mw in range(2):
            for dh in range(2):
                for mh in range(2):
                    at = (2 * mh + mw) * 64
                    for ew in range(2):
                        kw = 2 * dw + mw - 2 * ew
                        value = w_down2[2 * dh + mh, kw] if 0 <= kw < 4 else jnp.zeros((64, L), BF16)
                        wd2[dw, dh, at:at + 64, L * ew:L * ew + L] = value
    for dw in range(2):
        for mw in range(2):
            for kh in range(3):
                for ew in range(2):
                    kw = 2 * dw + mw - ew
                    value = w_conv2[kh, kw] if 0 <= kw < 3 else jnp.zeros((L, L), BF16)
                    wc2[dw, kh, L * mw:L * mw + L, L * ew:L * ew + L] = value


def solution(mesh):
    rows, cols = mesh.shape['row'], mesh.shape['col']

    def local(images, w_down1, b_down1, w_conv1, b_conv1, w_down2, b_down2, w_conv2, b_conv2, w_down3, b_down3, w_conv3, b_conv3):
        x = jnp.transpose(images, (0, 3, 1, 2))

        def row(b):
            return b.reshape(1, -1)

        def act(w, h):
            return pltpu.VMEM((w, h, N, C), BF16)

        vmem = pl.BlockSpec(memory_space=pltpu.VMEM)
        hbm = pl.BlockSpec(memory_space=pl.ANY)
        strip = pltpu.VMEM((12, 8, PIX), BF16)
        weight_in = [pltpu.VMEM(w.shape, BF16) for w in (w_conv1, w_down2, w_conv2)]
        weights = [pltpu.VMEM(shape, BF16) for shape in
                   ((C, C), (2, 2, C, C), (3, 2, C, C), (2, 3, C, C), w_down3.shape, w_conv3.shape)]
        dma = pltpu.SemaphoreType.DMA
        out = pl.pallas_call(
            functools.partial(body, rows, cols),
            out_shape=jax.ShapeDtypeStruct((N, N, N, C), BF16),
            in_specs=[hbm, vmem, vmem] + [hbm, vmem] * 5,
            out_specs=hbm,
            scratch_shapes=[pltpu.VMEM((N, 3, L, L), BF16)] + weight_in + [pltpu.VMEM((N, 3, 8, L), BF16)] * 2
            + [pltpu.VMEM((3, 17 * (L + N), L), F32), pltpu.VMEM((12, 144, PIX), F32)] + [strip] * 4
            + [act(34, 34), act(33, 33), act(18, 36), act(17, 34), act(18, 18)] + weights
            + [pltpu.VMEM((8, C), F32), pltpu.VMEM((6, 2, 17 * N, L), F32), act(N, N), dma((28,)), dma((28,)), dma((6,)), dma((4,))],
            compiler_params=pltpu.CompilerParams(collective_id=0, has_side_effects=True, vmem_limit_bytes=66_000_000),
            name='encoder',
        )(x, jnp.transpose(w_down1, (0, 2, 1, 3)), row(b_down1), w_conv1, row(b_conv1), w_down2, row(b_down2), w_conv2, row(b_conv2),
          w_down3, row(b_down3), w_conv3, row(b_conv3))
        return pl.pallas_call(
            hand_on,
            out_shape=jax.ShapeDtypeStruct(out.shape, BF16),
            in_specs=[hbm],
            out_specs=hbm,
            scratch_shapes=[act(N, N), dma((8,)), dma((8,))],
            name='hand_on',
        )(out)

    tile_spec = P('batch', 'row', 'col', None)
    return jax.shard_map(local, mesh=mesh, in_specs=(tile_spec,) + (P(),) * 12, out_specs=tile_spec, check_vma=False)
```

```python
import functools

import jax
import jax.numpy as jnp
from jax import lax
from jax.experimental import pallas as pl
from jax.experimental.pallas import tpu as pltpu
from jax.sharding import PartitionSpec as P

MESH = pl.DeviceIdType.MESH
F32 = jnp.float32
BF16 = jnp.bfloat16

N = 16
L = 128
C = 256
PIX = 640
HALF = 64
PITCH = 17


def body(rows, cols, x_hbm, w_down1, b_down1, w_conv1_hbm, b_conv1, w_down2_hbm, b_down2, w_conv2_hbm, b_conv2, w_down3, b_down3,
         w_conv3, b_conv3, out_hbm, x_ref, w_conv1, w_down2, w_conv2, top, bot, xs, tt, kept, send_l, send_r, recv_l, recv_r, y1, z1, y2, z2, y3,
         wd1, wc1, wd2, wc2, wd3, wc3, biases, turn, out_ref, ssem, rsem, wsem, osem):
    r = lax.axis_index('row')
    c = lax.axis_index('col')
    has_up, has_dn = r > 0, r < rows - 1
    has_lf, has_rt = c > 0, c < cols - 1

    loads = [pltpu.make_async_copy(src, dst, wsem.at[k]) for k, (src, dst) in enumerate((
        (x_hbm, x_ref), (w_conv1_hbm, w_conv1), (w_down2_hbm, w_down2), (w_conv2_hbm, w_conv2), (w_down3, wd3), (w_conv3, wc3)))]
    for copy in loads:
        copy.start()

    neighbours = []
    for dr in (-1, 0, 1):
        for dc in (-1, 0, 1):
            if dr == 0 and dc == 0:
                continue
            there = None
            if dr:
                there = has_up if dr < 0 else has_dn
            if dc:
                side = has_lf if dc < 0 else has_rt
                there = side if there is None else jnp.logical_and(there, side)
            neighbours.append((dr, dc, there))

    def device(dr, dc):
        return {'row': r + dr, 'col': c + dc}

    barrier = pltpu.get_barrier_semaphore()
    for dr, dc, there in neighbours:
        if dr and dc:
            continue

        @pl.when(there)
        def _():
            pl.semaphore_signal(barrier, inc=1, device_id=device(dr, dc), device_id_type=MESH)
    pl.semaphore_wait(barrier, sum(t.astype(jnp.int32) for t in (has_up, has_dn, has_lf, has_rt)))

    def remote(src, dst, k, dr, dc):
        return pltpu.make_async_remote_copy(src_ref=src, dst_ref=dst, send_sem=ssem.at[k], recv_sem=rsem.at[k],
                                            device_id=device(dr, dc), device_id_type=MESH)

    to_dn = remote(x_ref.at[:, :, L - 8:L], top, 0, 1, 0)
    to_up = remote(x_ref.at[:, :, 0:8], bot, 1, -1, 0)
    loads[0].wait()

    @pl.when(has_dn)
    def _():
        to_dn.start()

    @pl.when(has_up)
    def _():
        to_up.start()

    def clear(ref, there, index):
        @pl.when(jnp.logical_not(there))
        def _():
            ref[index] = jnp.zeros_like(ref[index])

    every = slice(None)
    clear(top, has_up, (every,))
    clear(bot, has_dn, (every,))
    pack_down1(w_down1, wd1)
    for k, b in enumerate((b_down1, b_conv1, b_down2, b_conv2, b_down3, b_conv3)):
        biases[k:k + 1, :] = jnp.concatenate([b[...]] * (C // b.shape[1]), axis=1)

    def gather(ch, src, h, size):
        for n in range(N):
            xs[ch, pl.ds(PITCH * (h + 8) + n, size, stride=PITCH), :] = src[n, ch].astype(F32)

    def put(ch, g):
        for u in range(4):
            pieces = []
            for k in range(8):
                at = PITCH * (32 * g + u + 3 + 4 * k)
                pieces.append(xs[ch, at:at + N, :] if at < PITCH * (L + N) else jnp.zeros((N, L), F32))
            t = jnp.transpose(jnp.concatenate(pieces, axis=0))
            cu = ch * 4 + u
            lanes = slice(g * L, g * L + L)
            tt[cu, 5:5 + L, lanes] = t
            send_l[cu, :, lanes] = t[0:8].astype(BF16)
            send_r[cu, :, lanes] = t[L - 8:L].astype(BF16)

    def inner(ch, _):
        gather(ch, x_ref, 0, L)
        for g in (1, 2, 3):
            put(ch, g)
        return 0

    lax.fori_loop(0, 3, inner, 0)

    def dots(pairs):
        acc = None
        for lhs, w in pairs:
            d = jnp.dot(lhs, w, preferred_element_type=F32)
            acc = d if acc is None else acc + d
        return acc

    def finish(acc, k, shape):
        return jnp.maximum(acc + biases[k:k + 1, :], 0.0).astype(BF16).reshape(shape)

    def window(k, e, lanes):
        size = sum(last - first for first, last in lanes)
        win = [tt[:, 8 * k:8 * k + N, first:last][:, 4 * e:4 * e + 8].reshape(96, last - first) for first, last in lanes]
        xt = jnp.transpose(jnp.concatenate(win, axis=1).astype(BF16))
        return jnp.concatenate([xt, jnp.zeros((size, L - 96), BF16)], axis=1)

    def down1(k):
        m = 34 * N
        for e in range(2):
            xb = window(k, e, [(0, PIX)])
            lhs = jnp.concatenate([xb[0:m], xb[N:N + m]], axis=1)
            y1[2 * k + e] = finish(dots([(lhs, wd1[...])]), 0, (34, N, C))

    def down1_inner(k):
        m = 23 * N
        for e in range(2):
            xb = window(k, e, [(L, 4 * L)])
            kept[2 * k + e, 0] = xb[0:N]
            kept[2 * k + e, 1] = xb[m:m + N]
            lhs = jnp.concatenate([xb[0:m], xb[N:N + m]], axis=1)
            y1[2 * k + e, 8:31] = finish(dots([(lhs, wd1[...])]), 0, (23, N, C))

    def down1_outer(k):
        lhs = []
        for e in range(2):
            xb = window(k, e, [(0, L), (4 * L, PIX)])
            this = jnp.concatenate([xb[0:L], kept[2 * k + e, 1], xb[L:L + 2 * N]], axis=0)
            below = jnp.concatenate([xb[N:L], kept[2 * k + e, 0], xb[L:L + 3 * N]], axis=0)
            lhs.append(jnp.concatenate([this, below], axis=1))
        res = finish(dots([(jnp.concatenate(lhs, axis=0), wd1[...])]), 0, (2, 11, N, C))
        y1[2 * k:2 * k + 2, 0:8] = res[:, 0:8]
        y1[2 * k:2 * k + 2, 31:34] = res[:, 8:11]

    for k in range(1, N):
        down1_inner(k)

    @pl.when(has_up)
    def _():
        to_up.wait_send()
        to_dn.wait_recv()

    @pl.when(has_dn)
    def _():
        to_dn.wait_send()
        to_up.wait_recv()

    def outer(ch, _):
        gather(ch, top, -8, 8)
        gather(ch, bot, L, 8)
        for g in (0, 4):
            put(ch, g)
        return 0

    lax.fori_loop(0, 3, outer, 0)

    to_lf = remote(send_l, recv_r, 2, 0, -1)
    to_rt = remote(send_r, recv_l, 3, 0, 1)

    @pl.when(has_lf)
    def _():
        to_lf.start()

    @pl.when(has_rt)
    def _():
        to_rt.start()

    def loop(start, stop, unroll, step):
        assert (stop - start) % unroll == 0

        def run(t, _):
            for e in range(unroll):
                step(start + t * unroll + e)
            return 0

        lax.fori_loop(0, (stop - start) // unroll, run, 0)

    def conv1(b):
        pairs = [(y1[b + dw, dh:dh + 33].reshape(33 * N, C), wc1[dw, dh]) for dw in range(2) for dh in range(2)]
        z1[b] = finish(dots(pairs), 1, (33, N, C))

    for copy in loads[1:4]:
        copy.wait()
    pack_conv1(w_conv1, wc1)
    for k in range(1, N):
        down1_outer(k)
    clear(y1, has_up, (slice(2, 32), slice(0, 1)))
    clear(y1, has_dn, (slice(2, 32), slice(33, 34)))
    loop(2, 30, 14, conv1)

    @pl.when(has_lf)
    def _():
        to_lf.wait_send()
        to_rt.wait_recv()

    @pl.when(has_rt)
    def _():
        to_rt.wait_send()
        to_lf.wait_recv()

    clear(recv_l, has_lf, (every,))
    clear(recv_r, has_rt, (every,))
    tt[:, 0:5, :] = recv_l[...].astype(F32)[:, 3:8]
    tt[:, 5 + L:13 + L, :] = recv_r[...].astype(F32)
    down1(0)
    down1(N)
    for part in (slice(0, 2), slice(32, 34)):
        clear(y1, has_up, (part, slice(0, 1)))
        clear(y1, has_dn, (part, slice(33, 34)))
    clear(y1, has_lf, (slice(0, 1),))
    clear(y1, has_rt, (slice(33, 34),))
    pack_stage2(w_down2, w_conv2, wd2, wc2)
    for b in (0, 1, 30, 31, 32):
        conv1(b)
    clear(z1, has_up, (every, slice(0, 1), every, slice(0, L)))
    clear(z1, has_dn, (every, slice(32, 33), every, slice(L, C)))
    for half in (0, L):
        clear(z1, has_lf, (slice(0, 1), every, every, slice(half, half + HALF)))
        clear(z1, has_rt, (slice(32, 33), every, every, slice(half + HALF, half + L)))

    def edge(d, around, size, step):
        first, last = around, around + size
        if d == 0:
            return slice(first, last), slice(first, last)
        if d > 0:
            return slice(last - step, last), slice(first - step, first)
        return slice(first, first + step), slice(last, last + step)

    def start(copies):
        for copy, there, _ in copies:
            @pl.when(there)
            def _():
                copy.start()

    def finished(copies):
        for copy, there, back in copies:
            @pl.when(there)
            def _():
                copy.wait_send()
                back.wait_recv()

    def exchange(ref, k0, w_axis, h_axis, wanted):
        made = {}
        for k, (dr, dc, there) in enumerate(neighbours):
            if wanted(dr, dc):
                (ws, wd), (hs, hd) = edge(dc, *w_axis), edge(dr, *h_axis)
                made[k] = (remote(ref.at[ws, hs], ref.at[wd, hd], k0 + k, dr, dc), there)
        return [(copy, there, made[7 - k][0]) for k, (copy, there) in made.items()]

    def sideways(dr, dc):
        return dc != 0

    def upright(dr, dc):
        return dc == 0

    y2_cols = exchange(y2, 4, (1, N, 1), (2, 32, 2), sideways)
    y2_rows = [exchange(y2, k0, (w0, 8, 1), (2, 32, 2), upright) for k0, w0 in ((4, 1), (12, 9))]
    y3_cols = exchange(y3, 20, (1, N, 1), (1, N, 1), sideways)
    y3_rows = exchange(y3, 20, (1, N, 1), (1, N, 1), upright)

    def down2(p):
        pairs = [(z1[2 * p + dw, dh:dh + 32].reshape(32 * N, C), wd2[dw, dh]) for dw in range(3) for dh in range(2)]
        y2[p + 1, 2:34] = finish(dots(pairs), 2, (32, N, C))

    def conv2(q):
        pairs = [(y2[q + dw, dh:dh + 34].reshape(34 * N, C), wc2[dw, dh]) for dw in range(2) for dh in range(3)]
        z2[q] = finish(dots(pairs), 3, (34, N, C))

    def conv2_inner(q):
        pairs = [(y2[q + dw, dh + 2:dh + 32].reshape(30 * N, C), wc2[dw, dh]) for dw in range(2) for dh in range(3)]
        z2[q, 2:32] = finish(dots(pairs), 3, (30, N, C))

    def conv2_rest(first, last):
        pairs = []
        for dw in range(2):
            for dh in range(3):
                lhs = [y2[q + dw, h + dh:h + dh + 2].reshape(2 * N, C) for q in range(first, last) for h in (0, 32)]
                pairs.append((jnp.concatenate(lhs, axis=0), wc2[dw, dh]))
        res = finish(dots(pairs), 3, (last - first, 4, N, C))
        z2[first:last, 0:2] = res[:, 0:2]
        z2[first:last, 32:34] = res[:, 2:4]

    for ref, step, last in ((y2, 2, 34), (y3, 1, 17)):
        clear(ref, has_up, (every, slice(0, step)))
        clear(ref, has_dn, (every, slice(last, last + step)))
        clear(ref, has_lf, (slice(0, 1),))
        clear(ref, has_rt, (slice(17, 18),))
    down2(0)
    down2(N - 1)
    start(y2_cols)
    loop(1, 8, 7, down2)
    start(y2_rows[0])
    loop(8, N - 1, 7, down2)
    start(y2_rows[1])
    for q in range(3, 12):
        conv2_inner(q)
    for copies in (*y2_rows, y2_cols):
        finished(copies)
    outer_q = (slice(0, 3), slice(14, 17))
    for part in outer_q:
        for q in range(part.start, part.stop):
            conv2(q)
    for part in outer_q:
        clear(z2, has_up, (part, slice(0, 1)))
        clear(z2, has_dn, (part, slice(33, 34)))
    clear(z2, has_lf, (slice(0, 1), every, every, slice(0, L)))
    clear(z2, has_rt, (slice(N, N + 1), every, every, slice(L, C)))
    for copy in loads[4:]:
        copy.wait()

    def down3(k):
        pairs = []
        for dw in range(2):
            for dh in range(4):
                lhs = [z2[2 * k + e + dw, dh + 2 * i] for e in range(2) for i in range(N)]
                pairs.append((jnp.concatenate(lhs, axis=0), wd3[dh, 2 * dw:2 * dw + 2].reshape(C, C)))
        y3[pl.ds(2 * k + 1, 2), 1:17] = finish(dots(pairs), 4, (2, N, N, C))

    down3(0)
    down3(7)
    start(y3_cols)
    conv2_inner(12)
    conv2_inner(13)
    conv2_rest(3, 14)
    clear(z2, has_up, (slice(3, 14), slice(0, 1)))
    clear(z2, has_dn, (slice(3, 14), slice(33, 34)))
    for k in range(1, 7):
        down3(k)
    start(y3_rows)

    def conv3(pair, slot):
        pairs = []
        for dw in range(3):
            for dh in range(3):
                lhs = [y3[dw:dw + N, i + dh].reshape(C, C) for i in pair]
                pairs.append((jnp.concatenate(lhs, axis=0), wc3[dh, dw]))
        res = jnp.maximum(dots(pairs) + biases[5:6, :], 0.0)
        for e, i in enumerate(pair):
            at = 2 * slot + e
            for j in range(N):
                for half in range(2):
                    row = (N * e + j) * N
                    turn[at, half, pl.ds(j, N, stride=PITCH), :] = res[row:row + N, half * L:half * L + L]
            for n in range(N):
                both = [turn[at, half, PITCH * n:PITCH * n + N, :] for half in range(2)]
                out_ref[n, i] = jnp.concatenate(both, axis=1).astype(BF16)

    def put_out(i, size, k):
        return pltpu.make_async_copy(out_ref.at[:, pl.ds(i, size)], out_hbm.at[:, pl.ds(i, size)], osem.at[k])

    finished(y3_cols)

    def conv3_inner(t, _):
        for e in range(3):
            i = 6 * t + 2 * e + 1
            conv3((i, i + 1), e)
        put_out(6 * t + 1, 6, t).start()
        return 0

    lax.fori_loop(0, 2, conv3_inner, 0)
    finished(y3_rows)
    last = [put_out(13, 2, 2), put_out(0, 1, 3), put_out(15, 1, 4)]
    conv3((13, 14), 0)
    last[0].start()
    conv3((0, 15), 1)
    for copy in last[1:]:
        copy.start()
    for copy in (put_out(1, 6, 0), put_out(7, 6, 1), *last):
        copy.wait()


def hand_on(src, dst, held, isem, osem):
    parts = [pl.ds(2 * k, 2) for k in range(8)]
    reads = [pltpu.make_async_copy(src.at[p], held.at[p], isem.at[k]) for k, p in enumerate(parts)]
    writes = [pltpu.make_async_copy(held.at[p], dst.at[p], osem.at[k]) for k, p in enumerate(parts)]
    for copy in reads:
        copy.start()
    for read, write in zip(reads, writes):
        read.wait()
        write.start()
    for copy in writes:
        copy.wait()


def pack_down1(w_down1, wd1):
    for dh in range(2):
        blocks = []
        for ch in range(3):
            for u in range(4):
                across = []
                for eh in range(2):
                    for ew in range(2):
                        kh = 4 * dh + u - 2 * eh
                        if 0 <= kh < 4:
                            down = [w_down1[kh, ch].astype(F32), jnp.zeros((4 - 2 * ew, HALF), F32)]
                            across.append(jnp.concatenate(([jnp.zeros((2, HALF), F32)] if ew else []) + down, axis=0))
                        else:
                            across.append(jnp.zeros((8, HALF), F32))
                blocks.append(jnp.concatenate(across, axis=1))
        blocks.append(jnp.zeros((32, C), F32))
        wd1[L * dh:L * dh + L, :] = jnp.concatenate(blocks, axis=0).astype(BF16)


def pack_conv1(w_conv1, wc1):
    for dw in range(2):
        for mw in range(2):
            for dh in range(2):
                for mh in range(2):
                    across = []
                    for eh in range(2):
                        for ew in range(2):
                            kh, kw = 2 * dh + mh - eh, 2 * dw + mw - ew
                            inside = 0 <= kh < 3 and 0 <= kw < 3
                            across.append(w_conv1[kh, kw] if inside else jnp.zeros((HALF, HALF), BF16))
                    at = (2 * mh + mw) * HALF
                    wc1[dw, dh, at:at + HALF, :] = jnp.concatenate(across, axis=1)


def pack_stage2(w_down2, w_conv2, wd2, wc2):
    for dw in range(3):
        for mw in range(2):
            for dh in range(2):
                for mh in range(2):
                    at = (2 * mh + mw) * HALF
                    for ew in range(2):
                        kw = 2 * dw + mw - 2 * ew
                        value = w_down2[2 * dh + mh, kw] if 0 <= kw < 4 else jnp.zeros((HALF, L), BF16)
                        wd2[dw, dh, at:at + HALF, L * ew:L * ew + L] = value
    for dw in range(2):
        for mw in range(2):
            for kh in range(3):
                for ew in range(2):
                    kw = 2 * dw + mw - ew
                    value = w_conv2[kh, kw] if 0 <= kw < 3 else jnp.zeros((L, L), BF16)
                    wc2[dw, kh, L * mw:L * mw + L, L * ew:L * ew + L] = value


def solution(mesh):
    rows, cols = mesh.shape['row'], mesh.shape['col']

    def local(images, w_down1, b_down1, w_conv1, b_conv1, w_down2, b_down2, w_conv2, b_conv2, w_down3, b_down3, w_conv3, b_conv3):
        x = jnp.transpose(images, (0, 3, 1, 2))

        def row(b):
            return b.reshape(1, -1)

        def act(w, h):
            return pltpu.VMEM((w, h, N, C), BF16)

        vmem = pl.BlockSpec(memory_space=pltpu.VMEM)
        hbm = pl.BlockSpec(memory_space=pl.ANY)
        strip = pltpu.VMEM((12, 8, PIX), BF16)
        weight_in = [pltpu.VMEM(w.shape, BF16) for w in (w_conv1, w_down2, w_conv2)]
        weights = [pltpu.VMEM(shape, BF16) for shape in
                   ((C, C), (2, 2, C, C), (3, 2, C, C), (2, 3, C, C), w_down3.shape, w_conv3.shape)]
        dma = pltpu.SemaphoreType.DMA
        out = pl.pallas_call(
            functools.partial(body, rows, cols),
            out_shape=jax.ShapeDtypeStruct((N, N, N, C), BF16),
            in_specs=[hbm, vmem, vmem] + [hbm, vmem] * 5,
            out_specs=hbm,
            scratch_shapes=[pltpu.VMEM((N, 3, L, L), BF16)] + weight_in + [pltpu.VMEM((N, 3, 8, L), BF16)] * 2
            + [pltpu.VMEM((3, PITCH * (L + N), L), F32), pltpu.VMEM((12, 144, PIX), F32), pltpu.VMEM((34, 2, N, L), BF16)] + [strip] * 4
            + [act(34, 34), act(33, 33), act(18, 36), act(17, 34), act(18, 18)] + weights
            + [pltpu.VMEM((8, C), F32), pltpu.VMEM((6, 2, PITCH * N, L), F32), act(N, N), dma((28,)), dma((28,)), dma((6,)), dma((5,))],
            compiler_params=pltpu.CompilerParams(collective_id=0, has_side_effects=True, vmem_limit_bytes=66_000_000),
            name='encoder',
        )(x, jnp.transpose(w_down1, (0, 2, 1, 3)), row(b_down1), w_conv1, row(b_conv1), w_down2, row(b_down2), w_conv2, row(b_conv2),
          w_down3, row(b_down3), w_conv3, row(b_conv3))
        return pl.pallas_call(
            hand_on,
            out_shape=jax.ShapeDtypeStruct(out.shape, BF16),
            in_specs=[hbm],
            out_specs=hbm,
            scratch_shapes=[act(N, N), dma((8,)), dma((8,))],
            name='hand_on',
        )(out)

    tile_spec = P('batch', 'row', 'col', None)
    return jax.shard_map(local, mesh=mesh, in_specs=(tile_spec,) + (P(),) * 12, out_specs=tile_spec, check_vma=False)
```

```python
import functools

import jax
import jax.numpy as jnp
from jax import lax
from jax.experimental import pallas as pl
from jax.experimental.pallas import tpu as pltpu
from jax.sharding import PartitionSpec as P

MESH = pl.DeviceIdType.MESH
F32 = jnp.float32
BF16 = jnp.bfloat16

N = 16
L = 128
C = 256
PIX = 640
HALF = 64
PITCH = 17


def body(rows, cols, x_hbm, w_down1, b_down1, w_conv1_hbm, b_conv1, w_down2_hbm, b_down2, w_conv2_hbm, b_conv2, w_down3, b_down3,
         w_conv3, b_conv3, out_hbm, x_ref, w_conv1, w_down2, w_conv2, top, bot, xs, tt, kept, send_l, send_r, recv_l, recv_r, y1, z1, y2, z2, y3,
         wd1, wc1, wd2, wc2, wd3, wc3, biases, turn, out_ref, ssem, rsem, wsem, osem):
    r = lax.axis_index('row')
    c = lax.axis_index('col')
    has_up, has_dn = r > 0, r < rows - 1
    has_lf, has_rt = c > 0, c < cols - 1

    loads = [pltpu.make_async_copy(src, dst, wsem.at[k]) for k, (src, dst) in enumerate((
        (x_hbm, x_ref), (w_conv1_hbm, w_conv1), (w_down2_hbm, w_down2), (w_conv2_hbm, w_conv2), (w_down3, wd3), (w_conv3, wc3)))]
    for copy in loads:
        copy.start()

    neighbours = []
    for dr in (-1, 0, 1):
        for dc in (-1, 0, 1):
            if dr == 0 and dc == 0:
                continue
            there = None
            if dr:
                there = has_up if dr < 0 else has_dn
            if dc:
                side = has_lf if dc < 0 else has_rt
                there = side if there is None else jnp.logical_and(there, side)
            neighbours.append((dr, dc, there))

    def device(dr, dc):
        return {'row': r + dr, 'col': c + dc}

    barrier = pltpu.get_barrier_semaphore()
    for dr, dc, there in neighbours:
        if dr and dc:
            continue

        @pl.when(there)
        def _():
            pl.semaphore_signal(barrier, inc=1, device_id=device(dr, dc), device_id_type=MESH)
    pl.semaphore_wait(barrier, sum(t.astype(jnp.int32) for t in (has_up, has_dn, has_lf, has_rt)))

    def remote(src, dst, k, dr, dc):
        return pltpu.make_async_remote_copy(src_ref=src, dst_ref=dst, send_sem=ssem.at[k], recv_sem=rsem.at[k],
                                            device_id=device(dr, dc), device_id_type=MESH)

    to_dn = remote(x_ref.at[:, :, L - 8:L], top, 0, 1, 0)
    to_up = remote(x_ref.at[:, :, 0:8], bot, 1, -1, 0)
    loads[0].wait()

    @pl.when(has_dn)
    def _():
        to_dn.start()

    @pl.when(has_up)
    def _():
        to_up.start()

    up, dn, lf, rt = (jnp.where(there, jnp.inf, 0.0).astype(F32) for there in (has_up, has_dn, has_lf, has_rt))

    def clear(ref, there, index):
        @pl.when(jnp.logical_not(there))
        def _():
            ref[index] = jnp.zeros_like(ref[index])

    every = slice(None)
    clear(top, has_up, (every,))
    clear(bot, has_dn, (every,))
    clear(recv_l, has_lf, (every,))
    clear(recv_r, has_rt, (every,))
    for ref, step, last in ((y2, 2, 34), (y3, 1, N + 1)):
        clear(ref, has_up, (every, slice(0, step)))
        clear(ref, has_dn, (every, slice(last, last + step)))
        clear(ref, has_lf, (slice(0, 1),))
        clear(ref, has_rt, (slice(N + 1, N + 2),))
    pack_down1(w_down1, wd1)
    for k, b in enumerate((b_down1, b_conv1, b_down2, b_conv2, b_down3, b_conv3)):
        biases[k:k + 1, :] = jnp.concatenate([b[...]] * (C // b.shape[1]), axis=1)

    def gather(ch, src, h, size):
        for n in range(N):
            xs[ch, pl.ds(PITCH * (h + 8) + n, size, stride=PITCH), :] = src[n, ch].astype(F32)

    def put(ch, g):
        for u in range(4):
            pieces = []
            for k in range(8):
                at = PITCH * (32 * g + u + 3 + 4 * k)
                pieces.append(xs[ch, at:at + N, :] if at < PITCH * (L + N) else jnp.zeros((N, L), F32))
            t = jnp.transpose(jnp.concatenate(pieces, axis=0))
            cu = ch * 4 + u
            lanes = slice(g * L, g * L + L)
            tt[cu, 5:5 + L, lanes] = t
            send_l[cu, :, lanes] = t[0:8].astype(BF16)
            send_r[cu, :, lanes] = t[L - 8:L].astype(BF16)

    def inner(ch, _):
        gather(ch, x_ref, 0, L)
        for g in (1, 2, 3):
            put(ch, g)
        return 0

    lax.fori_loop(0, 3, inner, 0)

    def dots(pairs):
        acc = None
        for lhs, w in pairs:
            d = jnp.dot(lhs, w, preferred_element_type=F32)
            acc = d if acc is None else acc + d
        return acc

    def relu(acc, k, shape):
        return jnp.maximum(acc + biases[k:k + 1, :], 0.0).reshape(shape)

    def finish(acc, k, shape):
        return relu(acc, k, shape).astype(BF16)

    def bound(v, inside, first=0, last=C):
        parts = [v[..., :first], jnp.minimum(v[..., first:last], inside), v[..., last:]]
        return jnp.concatenate([p for p in parts if p.shape[-1]], axis=-1)

    def put_rows(ref, w, v, first=(0, C), last=(0, C)):
        h = v.shape[0]
        ref[w, 0:1] = bound(v[0:1], up, *first).astype(BF16)
        ref[w, 1:h - 1] = v[1:h - 1].astype(BF16)
        ref[w, h - 1:h] = bound(v[h - 1:h], dn, *last).astype(BF16)

    def window(k, e, lanes):
        size = sum(last - first for first, last in lanes)
        win = [tt[:, 8 * k:8 * k + N, first:last][:, 4 * e:4 * e + 8].reshape(96, last - first) for first, last in lanes]
        xt = jnp.transpose(jnp.concatenate(win, axis=1).astype(BF16))
        return jnp.concatenate([xt, jnp.zeros((size, L - 96), BF16)], axis=1)

    def down1(k):
        m = 34 * N
        for e in range(2):
            xb = window(k, e, [(0, PIX)])
            lhs = jnp.concatenate([xb[0:m], xb[N:N + m]], axis=1)
            v = relu(dots([(lhs, wd1[...])]), 0, (34, N, C))
            if 2 * k + e in (0, 33):
                v = jnp.minimum(v, rt if k else lf)
            put_rows(y1, 2 * k + e, v)

    def down1_inner(k):
        m = 23 * N
        for e in range(2):
            xb = window(k, e, [(L, 4 * L)])
            kept[2 * k + e, 0] = xb[0:N]
            kept[2 * k + e, 1] = xb[m:m + N]
            lhs = jnp.concatenate([xb[0:m], xb[N:N + m]], axis=1)
            y1[2 * k + e, 8:31] = finish(dots([(lhs, wd1[...])]), 0, (23, N, C))

    def down1_outer(k):
        lhs = []
        for e in range(2):
            xb = window(k, e, [(0, L), (4 * L, PIX)])
            this = jnp.concatenate([xb[0:L], kept[2 * k + e, 1], xb[L:L + 2 * N]], axis=0)
            below = jnp.concatenate([xb[N:L], kept[2 * k + e, 0], xb[L:L + 3 * N]], axis=0)
            lhs.append(jnp.concatenate([this, below], axis=1))
        v = relu(dots([(jnp.concatenate(lhs, axis=0), wd1[...])]), 0, (2, 11, N, C))
        both = slice(2 * k, 2 * k + 2)
        y1[both, 0:1] = bound(v[:, 0:1], up).astype(BF16)
        y1[both, 1:8] = v[:, 1:8].astype(BF16)
        y1[both, 31:33] = v[:, 8:10].astype(BF16)
        y1[both, 33:34] = bound(v[:, 10:11], dn).astype(BF16)

    for k in range(1, N):
        down1_inner(k)

    @pl.when(has_up)
    def _():
        to_up.wait_send()
        to_dn.wait_recv()

    @pl.when(has_dn)
    def _():
        to_dn.wait_send()
        to_up.wait_recv()

    def outer(ch, _):
        gather(ch, top, -8, 8)
        gather(ch, bot, L, 8)
        for g in (0, 4):
            put(ch, g)
        return 0

    lax.fori_loop(0, 3, outer, 0)

    to_lf = remote(send_l, recv_r, 2, 0, -1)
    to_rt = remote(send_r, recv_l, 3, 0, 1)

    @pl.when(has_lf)
    def _():
        to_lf.start()

    @pl.when(has_rt)
    def _():
        to_rt.start()

    def loop(start, stop, unroll, step):
        assert (stop - start) % unroll == 0

        def run(t, _):
            for e in range(unroll):
                step(start + t * unroll + e)
            return 0

        lax.fori_loop(0, (stop - start) // unroll, run, 0)

    def conv1(b):
        pairs = [(y1[b + dw, dh:dh + 33].reshape(33 * N, C), wc1[dw, dh]) for dw in range(2) for dh in range(2)]
        v = relu(dots(pairs), 1, (33, N, C))
        if isinstance(b, int):
            for half in (0, L):
                if b == 0:
                    v = bound(v, lf, half, half + HALF)
                if b == 32:
                    v = bound(v, rt, half + HALF, half + L)
        put_rows(z1, b, v, (0, L), (L, C))

    for copy in loads[1:4]:
        copy.wait()
    pack_conv1(w_conv1, wc1)
    for k in range(1, N):
        down1_outer(k)
    loop(2, 18, 16, conv1)

    @pl.when(has_lf)
    def _():
        to_lf.wait_send()
        to_rt.wait_recv()

    @pl.when(has_rt)
    def _():
        to_rt.wait_send()
        to_lf.wait_recv()

    tt[:, 0:5, :] = recv_l[...].astype(F32)[:, 3:8]
    tt[:, 5 + L:13 + L, :] = recv_r[...].astype(F32)
    down1(0)
    down1(N)
    pack_stage2(w_down2, w_conv2, wd2, wc2)
    for b in (*range(18, 33), 0, 1):
        conv1(b)

    def edge(d, around, size, step):
        first, last = around, around + size
        if d == 0:
            return slice(first, last), slice(first, last)
        if d > 0:
            return slice(last - step, last), slice(first - step, first)
        return slice(first, first + step), slice(last, last + step)

    def start(copies):
        for copy, there, _ in copies:
            @pl.when(there)
            def _():
                copy.start()

    def finished(copies):
        for copy, there, back in copies:
            @pl.when(there)
            def _():
                copy.wait_send()
                back.wait_recv()

    def exchange(ref, k0, w_axis, h_axis, wanted):
        made = {}
        for k, (dr, dc, there) in enumerate(neighbours):
            if wanted(dr, dc):
                (ws, wd), (hs, hd) = edge(dc, *w_axis), edge(dr, *h_axis)
                made[k] = (remote(ref.at[ws, hs], ref.at[wd, hd], k0 + k, dr, dc), there)
        return [(copy, there, made[7 - k][0]) for k, (copy, there) in made.items()]

    def sideways(dr, dc):
        return dc != 0

    def upright(dr, dc):
        return dc == 0

    y2_cols = exchange(y2, 4, (1, N, 1), (2, 32, 2), sideways)
    y2_rows = [exchange(y2, k0, (w0, 8, 1), (2, 32, 2), upright) for k0, w0 in ((4, 1), (12, 9))]
    y3_cols = exchange(y3, 20, (1, N, 1), (1, N, 1), sideways)
    y3_rows = exchange(y3, 20, (1, N, 1), (1, N, 1), upright)

    def down2(p):
        pairs = [(z1[2 * p + dw, dh:dh + 32].reshape(32 * N, C), wd2[dw, dh]) for dw in range(3) for dh in range(2)]
        y2[p + 1, 2:34] = finish(dots(pairs), 2, (32, N, C))

    def conv2(q):
        pairs = [(y2[q + dw, dh:dh + 34].reshape(34 * N, C), wc2[dw, dh]) for dw in range(2) for dh in range(3)]
        v = relu(dots(pairs), 3, (34, N, C))
        if q == 0:
            v = bound(v, lf, 0, L)
        if q == N:
            v = bound(v, rt, L, C)
        put_rows(z2, q, v)

    def conv2_inner(q):
        pairs = [(y2[q + dw, dh + 2:dh + 32].reshape(30 * N, C), wc2[dw, dh]) for dw in range(2) for dh in range(3)]
        z2[q, 2:32] = finish(dots(pairs), 3, (30, N, C))

    def conv2_rest(first, last):
        pairs = []
        for dw in range(2):
            for dh in range(3):
                lhs = [y2[q + dw, h + dh:h + dh + 2].reshape(2 * N, C) for q in range(first, last) for h in (0, 32)]
                pairs.append((jnp.concatenate(lhs, axis=0), wc2[dw, dh]))
        v = relu(dots(pairs), 3, (last - first, 4, N, C))
        z2[first:last, 0:1] = bound(v[:, 0:1], up).astype(BF16)
        z2[first:last, 1:2] = v[:, 1:2].astype(BF16)
        z2[first:last, 32:33] = v[:, 2:3].astype(BF16)
        z2[first:last, 33:34] = bound(v[:, 3:4], dn).astype(BF16)

    down2(0)
    down2(N - 1)
    start(y2_cols)
    loop(1, 8, 7, down2)
    start(y2_rows[0])
    loop(8, N - 1, 7, down2)
    start(y2_rows[1])
    for q in range(3, 12):
        conv2_inner(q)
    for copies in (*y2_rows, y2_cols):
        finished(copies)
    for q in (0, 1, 2, 14, 15, N):
        conv2(q)
    for copy in loads[4:]:
        copy.wait()

    def down3(k):
        pairs = []
        for dw in range(2):
            for dh in range(4):
                lhs = [z2[2 * k + e + dw, dh + 2 * i] for e in range(2) for i in range(N)]
                pairs.append((jnp.concatenate(lhs, axis=0), wd3[dh, 2 * dw:2 * dw + 2].reshape(C, C)))
        y3[pl.ds(2 * k + 1, 2), 1:17] = finish(dots(pairs), 4, (2, N, N, C))

    down3(0)
    down3(7)
    start(y3_cols)
    conv2_inner(12)
    conv2_inner(13)
    conv2_rest(3, 14)
    for k in range(1, 7):
        down3(k)
    start(y3_rows)

    def conv3(pair, slot):
        pairs = []
        for dw in range(3):
            for dh in range(3):
                lhs = [y3[dw:dw + N, i + dh].reshape(C, C) for i in pair]
                pairs.append((jnp.concatenate(lhs, axis=0), wc3[dh, dw]))
        res = jnp.maximum(dots(pairs) + biases[5:6, :], 0.0)
        for e, i in enumerate(pair):
            at = 2 * slot + e
            for j in range(N):
                for half in range(2):
                    row = (N * e + j) * N
                    turn[at, half, pl.ds(j, N, stride=PITCH), :] = res[row:row + N, half * L:half * L + L]
            for n in range(N):
                both = [turn[at, half, PITCH * n:PITCH * n + N, :] for half in range(2)]
                out_ref[n, i] = jnp.concatenate(both, axis=1).astype(BF16)

    def put_out(i, size, k):
        return pltpu.make_async_copy(out_ref.at[:, pl.ds(i, size)], out_hbm.at[:, pl.ds(i, size)], osem.at[k])

    finished(y3_cols)

    def conv3_inner(t, _):
        for e in range(3):
            i = 6 * t + 2 * e + 1
            conv3((i, i + 1), e)
        put_out(6 * t + 1, 6, t).start()
        return 0

    lax.fori_loop(0, 2, conv3_inner, 0)
    finished(y3_rows)
    last = [put_out(13, 2, 2), put_out(0, 1, 3), put_out(15, 1, 4)]
    conv3((13, 14), 0)
    last[0].start()
    conv3((0, 15), 1)
    for copy in last[1:]:
        copy.start()
    for copy in (put_out(1, 6, 0), put_out(7, 6, 1), *last):
        copy.wait()


def hand_on(src, dst, held, isem, osem):
    parts = [pl.ds(2 * k, 2) for k in range(8)]
    reads = [pltpu.make_async_copy(src.at[p], held.at[p], isem.at[k]) for k, p in enumerate(parts)]
    writes = [pltpu.make_async_copy(held.at[p], dst.at[p], osem.at[k]) for k, p in enumerate(parts)]
    for copy in reads:
        copy.start()
    for read, write in zip(reads, writes):
        read.wait()
        write.start()
    for copy in writes:
        copy.wait()


def pack_down1(w_down1, wd1):
    for dh in range(2):
        blocks = []
        for ch in range(3):
            for u in range(4):
                across = []
                for eh in range(2):
                    for ew in range(2):
                        kh = 4 * dh + u - 2 * eh
                        if 0 <= kh < 4:
                            down = [w_down1[kh, ch].astype(F32), jnp.zeros((4 - 2 * ew, HALF), F32)]
                            across.append(jnp.concatenate(([jnp.zeros((2, HALF), F32)] if ew else []) + down, axis=0))
                        else:
                            across.append(jnp.zeros((8, HALF), F32))
                blocks.append(jnp.concatenate(across, axis=1))
        blocks.append(jnp.zeros((32, C), F32))
        wd1[L * dh:L * dh + L, :] = jnp.concatenate(blocks, axis=0).astype(BF16)


def pack_conv1(w_conv1, wc1):
    for dw in range(2):
        for mw in range(2):
            for dh in range(2):
                for mh in range(2):
                    across = []
                    for eh in range(2):
                        for ew in range(2):
                            kh, kw = 2 * dh + mh - eh, 2 * dw + mw - ew
                            inside = 0 <= kh < 3 and 0 <= kw < 3
                            across.append(w_conv1[kh, kw] if inside else jnp.zeros((HALF, HALF), BF16))
                    at = (2 * mh + mw) * HALF
                    wc1[dw, dh, at:at + HALF, :] = jnp.concatenate(across, axis=1)


def pack_stage2(w_down2, w_conv2, wd2, wc2):
    for dw in range(3):
        for mw in range(2):
            for dh in range(2):
                for mh in range(2):
                    at = (2 * mh + mw) * HALF
                    for ew in range(2):
                        kw = 2 * dw + mw - 2 * ew
                        value = w_down2[2 * dh + mh, kw] if 0 <= kw < 4 else jnp.zeros((HALF, L), BF16)
                        wd2[dw, dh, at:at + HALF, L * ew:L * ew + L] = value
    for dw in range(2):
        for mw in range(2):
            for kh in range(3):
                for ew in range(2):
                    kw = 2 * dw + mw - ew
                    value = w_conv2[kh, kw] if 0 <= kw < 3 else jnp.zeros((L, L), BF16)
                    wc2[dw, kh, L * mw:L * mw + L, L * ew:L * ew + L] = value


def solution(mesh):
    rows, cols = mesh.shape['row'], mesh.shape['col']

    def local(images, w_down1, b_down1, w_conv1, b_conv1, w_down2, b_down2, w_conv2, b_conv2, w_down3, b_down3, w_conv3, b_conv3):
        x = jnp.transpose(images, (0, 3, 1, 2))

        def row(b):
            return b.reshape(1, -1)

        def act(w, h):
            return pltpu.VMEM((w, h, N, C), BF16)

        vmem = pl.BlockSpec(memory_space=pltpu.VMEM)
        hbm = pl.BlockSpec(memory_space=pl.ANY)
        strip = pltpu.VMEM((12, 8, PIX), BF16)
        weight_in = [pltpu.VMEM(w.shape, BF16) for w in (w_conv1, w_down2, w_conv2)]
        weights = [pltpu.VMEM(shape, BF16) for shape in
                   ((C, C), (2, 2, C, C), (3, 2, C, C), (2, 3, C, C), w_down3.shape, w_conv3.shape)]
        dma = pltpu.SemaphoreType.DMA
        out = pl.pallas_call(
            functools.partial(body, rows, cols),
            out_shape=jax.ShapeDtypeStruct((N, N, N, C), BF16),
            in_specs=[hbm, vmem, vmem] + [hbm, vmem] * 5,
            out_specs=hbm,
            scratch_shapes=[pltpu.VMEM((N, 3, L, L), BF16)] + weight_in + [pltpu.VMEM((N, 3, 8, L), BF16)] * 2
            + [pltpu.VMEM((3, PITCH * (L + N), L), F32), pltpu.VMEM((12, 144, PIX), F32), pltpu.VMEM((34, 2, N, L), BF16)] + [strip] * 4
            + [act(34, 34), act(33, 33), act(18, 36), act(17, 34), act(18, 18)] + weights
            + [pltpu.VMEM((8, C), F32), pltpu.VMEM((6, 2, PITCH * N, L), F32), act(N, N), dma((28,)), dma((28,)), dma((6,)), dma((5,))],
            compiler_params=pltpu.CompilerParams(collective_id=0, has_side_effects=True, vmem_limit_bytes=66_000_000),
            name='encoder',
        )(x, jnp.transpose(w_down1, (0, 2, 1, 3)), row(b_down1), w_conv1, row(b_conv1), w_down2, row(b_down2), w_conv2, row(b_conv2),
          w_down3, row(b_down3), w_conv3, row(b_conv3))
        return pl.pallas_call(
            hand_on,
            out_shape=jax.ShapeDtypeStruct(out.shape, BF16),
            in_specs=[hbm],
            out_specs=hbm,
            scratch_shapes=[act(N, N), dma((8,)), dma((8,))],
            name='hand_on',
        )(out)

    tile_spec = P('batch', 'row', 'col', None)
    return jax.shard_map(local, mesh=mesh, in_specs=(tile_spec,) + (P(),) * 12, out_specs=tile_spec, check_vma=False)
```

```python
import functools

import jax
import jax.numpy as jnp
from jax import lax
from jax.experimental import pallas as pl
from jax.experimental.pallas import tpu as pltpu
from jax.sharding import PartitionSpec as P

MESH = pl.DeviceIdType.MESH
F32 = jnp.float32
BF16 = jnp.bfloat16

N = 16
L = 128
C = 256
PIX = 640
HALF = 64
PITCH = 17


def body(rows, cols, x_hbm, w_down1_hbm, w_conv1_hbm, w_down2_hbm, w_conv2_hbm, w_down3, w_conv3, *refs):
    b_hbm, out_hbm, bs = refs[:6], refs[6], refs[7:13]
    (x_ref, w_down1, w_conv1, w_down2, w_conv2, top, bot, xs, tt, kept, send_l, send_r, recv_l, recv_r, y1, z1, y2, z2,
     y3, wd1, wc1, wd2, wc2, wd3, wc3, biases, turn, out_ref, ssem, rsem, wsem, osem) = refs[13:]
    r = lax.axis_index('row')
    c = lax.axis_index('col')
    has_up, has_dn = r > 0, r < rows - 1
    has_lf, has_rt = c > 0, c < cols - 1

    loads = [pltpu.make_async_copy(src, dst, wsem.at[k]) for k, (src, dst) in enumerate((
        (x_hbm, x_ref), (w_conv1_hbm, w_conv1), (w_down2_hbm, w_down2), (w_conv2_hbm, w_conv2), (w_down3, wd3), (w_conv3, wc3),
        (w_down1_hbm, w_down1), *zip(b_hbm, bs)))]
    for copy in loads:
        copy.start()

    neighbours = []
    for dr in (-1, 0, 1):
        for dc in (-1, 0, 1):
            if dr == 0 and dc == 0:
                continue
            there = None
            if dr:
                there = has_up if dr < 0 else has_dn
            if dc:
                side = has_lf if dc < 0 else has_rt
                there = side if there is None else jnp.logical_and(there, side)
            neighbours.append((dr, dc, there))

    def device(dr, dc):
        return {'row': r + dr, 'col': c + dc}

    barrier = pltpu.get_barrier_semaphore()
    for dr, dc, there in neighbours:
        if dr and dc:
            continue

        @pl.when(there)
        def _():
            pl.semaphore_signal(barrier, inc=1, device_id=device(dr, dc), device_id_type=MESH)
    pl.semaphore_wait(barrier, sum(t.astype(jnp.int32) for t in (has_up, has_dn, has_lf, has_rt)))

    def remote(src, dst, k, dr, dc):
        return pltpu.make_async_remote_copy(src_ref=src, dst_ref=dst, send_sem=ssem.at[k], recv_sem=rsem.at[k],
                                            device_id=device(dr, dc), device_id_type=MESH)

    to_dn = remote(x_ref.at[:, :, L - 8:L], top, 0, 1, 0)
    to_up = remote(x_ref.at[:, :, 0:8], bot, 1, -1, 0)
    loads[0].wait()

    @pl.when(has_dn)
    def _():
        to_dn.start()

    @pl.when(has_up)
    def _():
        to_up.start()

    up, dn, lf, rt = (jnp.where(there, jnp.inf, 0.0).astype(F32) for there in (has_up, has_dn, has_lf, has_rt))

    def clear(ref, there, index):
        @pl.when(jnp.logical_not(there))
        def _():
            ref[index] = jnp.zeros_like(ref[index])

    every = slice(None)
    clear(top, has_up, (every,))
    clear(bot, has_dn, (every,))
    clear(recv_l, has_lf, (every,))
    clear(recv_r, has_rt, (every,))
    for ref, step, last in ((y2, 2, 34), (y3, 1, N + 1)):
        clear(ref, has_up, (every, slice(0, step)))
        clear(ref, has_dn, (every, slice(last, last + step)))
        clear(ref, has_lf, (slice(0, 1),))
        clear(ref, has_rt, (slice(N + 1, N + 2),))
    for copy in loads[6:]:
        copy.wait()
    pack_down1(w_down1, wd1)
    for k, b in enumerate(bs):
        biases[k:k + 1, :] = jnp.concatenate([b[...]] * (C // b.shape[1]), axis=1)

    def gather(ch, src, h, size):
        for n in range(N):
            xs[ch, pl.ds(PITCH * (h + 8) + n, size, stride=PITCH), :] = src[n, ch].astype(F32)

    def put(ch, g):
        for u in range(4):
            pieces = []
            for k in range(8):
                at = PITCH * (32 * g + u + 3 + 4 * k)
                pieces.append(xs[ch, at:at + N, :] if at < PITCH * (L + N) else jnp.zeros((N, L), F32))
            t = jnp.transpose(jnp.concatenate(pieces, axis=0))
            cu = ch * 4 + u
            lanes = slice(g * L, g * L + L)
            tt[cu, 5:5 + L, lanes] = t
            send_l[cu, :, lanes] = t[0:8].astype(BF16)
            send_r[cu, :, lanes] = t[L - 8:L].astype(BF16)

    def inner(ch, _):
        gather(ch, x_ref, 0, L)
        for g in (1, 2, 3):
            put(ch, g)
        return 0

    lax.fori_loop(0, 3, inner, 0)

    def dots(pairs):
        acc = None
        for lhs, w in pairs:
            d = jnp.dot(lhs, w, preferred_element_type=F32)
            acc = d if acc is None else acc + d
        return acc

    def relu(acc, k, shape):
        return jnp.maximum(acc + biases[k:k + 1, :], 0.0).reshape(shape)

    def finish(acc, k, shape):
        return relu(acc, k, shape).astype(BF16)

    def bound(v, inside, first=0, last=C):
        parts = [v[..., :first], jnp.minimum(v[..., first:last], inside), v[..., last:]]
        return jnp.concatenate([p for p in parts if p.shape[-1]], axis=-1)

    def put_rows(ref, w, v, first=(0, C), last=(0, C)):
        h = v.shape[0]
        ref[w, 0:1] = bound(v[0:1], up, *first).astype(BF16)
        ref[w, 1:h - 1] = v[1:h - 1].astype(BF16)
        ref[w, h - 1:h] = bound(v[h - 1:h], dn, *last).astype(BF16)

    def window(k, e, lanes):
        size = sum(last - first for first, last in lanes)
        win = [tt[:, 8 * k:8 * k + N, first:last][:, 4 * e:4 * e + 8].reshape(96, last - first) for first, last in lanes]
        xt = jnp.transpose(jnp.concatenate(win, axis=1).astype(BF16))
        return jnp.concatenate([xt, jnp.zeros((size, L - 96), BF16)], axis=1)

    def down1(k):
        m = 34 * N
        for e in range(2):
            xb = window(k, e, [(0, PIX)])
            lhs = jnp.concatenate([xb[0:m], xb[N:N + m]], axis=1)
            v = relu(dots([(lhs, wd1[...])]), 0, (34, N, C))
            if 2 * k + e in (0, 33):
                v = jnp.minimum(v, rt if k else lf)
            put_rows(y1, 2 * k + e, v)

    def down1_inner(k):
        m = 23 * N
        for e in range(2):
            xb = window(k, e, [(L, 4 * L)])
            kept[2 * k + e, 0] = xb[0:N]
            kept[2 * k + e, 1] = xb[m:m + N]
            lhs = jnp.concatenate([xb[0:m], xb[N:N + m]], axis=1)
            y1[2 * k + e, 8:31] = finish(dots([(lhs, wd1[...])]), 0, (23, N, C))

    def down1_outer(k):
        lhs = []
        for e in range(2):
            xb = window(k, e, [(0, L), (4 * L, PIX)])
            this = jnp.concatenate([xb[0:L], kept[2 * k + e, 1], xb[L:L + 2 * N]], axis=0)
            below = jnp.concatenate([xb[N:L], kept[2 * k + e, 0], xb[L:L + 3 * N]], axis=0)
            lhs.append(jnp.concatenate([this, below], axis=1))
        v = relu(dots([(jnp.concatenate(lhs, axis=0), wd1[...])]), 0, (2, 11, N, C))
        both = slice(2 * k, 2 * k + 2)
        y1[both, 0:1] = bound(v[:, 0:1], up).astype(BF16)
        y1[both, 1:8] = v[:, 1:8].astype(BF16)
        y1[both, 31:33] = v[:, 8:10].astype(BF16)
        y1[both, 33:34] = bound(v[:, 10:11], dn).astype(BF16)

    for k in range(1, N):
        down1_inner(k)

    @pl.when(has_up)
    def _():
        to_up.wait_send()
        to_dn.wait_recv()

    @pl.when(has_dn)
    def _():
        to_dn.wait_send()
        to_up.wait_recv()

    def outer(ch, _):
        gather(ch, top, -8, 8)
        gather(ch, bot, L, 8)
        for g in (0, 4):
            put(ch, g)
        return 0

    lax.fori_loop(0, 3, outer, 0)

    to_lf = remote(send_l, recv_r, 2, 0, -1)
    to_rt = remote(send_r, recv_l, 3, 0, 1)

    @pl.when(has_lf)
    def _():
        to_lf.start()

    @pl.when(has_rt)
    def _():
        to_rt.start()

    def loop(start, stop, unroll, step):
        assert (stop - start) % unroll == 0

        def run(t, _):
            for e in range(unroll):
                step(start + t * unroll + e)
            return 0

        lax.fori_loop(0, (stop - start) // unroll, run, 0)

    def conv1(b):
        pairs = [(y1[b + dw, dh:dh + 33].reshape(33 * N, C), wc1[dw, dh]) for dw in range(2) for dh in range(2)]
        v = relu(dots(pairs), 1, (33, N, C))
        if isinstance(b, int):
            for half in (0, L):
                if b == 0:
                    v = bound(v, lf, half, half + HALF)
                if b == 32:
                    v = bound(v, rt, half + HALF, half + L)
        put_rows(z1, b, v, (0, L), (L, C))

    for copy in loads[1:4]:
        copy.wait()
    pack_conv1(w_conv1, wc1)
    for k in range(1, N):
        down1_outer(k)
    loop(2, 18, 16, conv1)

    @pl.when(has_lf)
    def _():
        to_lf.wait_send()
        to_rt.wait_recv()

    @pl.when(has_rt)
    def _():
        to_rt.wait_send()
        to_lf.wait_recv()

    tt[:, 0:5, :] = recv_l[...].astype(F32)[:, 3:8]
    tt[:, 5 + L:13 + L, :] = recv_r[...].astype(F32)
    down1(0)
    down1(N)
    pack_stage2(w_down2, w_conv2, wd2, wc2)
    for b in (*range(18, 33), 0, 1):
        conv1(b)

    def edge(d, around, size, step):
        first, last = around, around + size
        if d == 0:
            return slice(first, last), slice(first, last)
        if d > 0:
            return slice(last - step, last), slice(first - step, first)
        return slice(first, first + step), slice(last, last + step)

    def start(copies):
        for copy, there, _ in copies:
            @pl.when(there)
            def _():
                copy.start()

    def finished(copies):
        for copy, there, back in copies:
            @pl.when(there)
            def _():
                copy.wait_send()
                back.wait_recv()

    def exchange(ref, k0, w_axis, h_axis, wanted):
        made = {}
        for k, (dr, dc, there) in enumerate(neighbours):
            if wanted(dr, dc):
                (ws, wd), (hs, hd) = edge(dc, *w_axis), edge(dr, *h_axis)
                made[k] = (remote(ref.at[ws, hs], ref.at[wd, hd], k0 + k, dr, dc), there)
        return [(copy, there, made[7 - k][0]) for k, (copy, there) in made.items()]

    def sideways(dr, dc):
        return dc != 0

    def upright(dr, dc):
        return dc == 0

    y2_cols = exchange(y2, 4, (1, N, 1), (2, 32, 2), sideways)
    y2_rows = [exchange(y2, k0, (w0, 8, 1), (2, 32, 2), upright) for k0, w0 in ((4, 1), (12, 9))]
    y3_cols = exchange(y3, 20, (1, N, 1), (1, N, 1), sideways)
    y3_rows = exchange(y3, 20, (1, N, 1), (1, N, 1), upright)

    def down2(p):
        pairs = [(z1[2 * p + dw, dh:dh + 32].reshape(32 * N, C), wd2[dw, dh]) for dw in range(3) for dh in range(2)]
        y2[p + 1, 2:34] = finish(dots(pairs), 2, (32, N, C))

    def conv2(q):
        pairs = [(y2[q + dw, dh:dh + 34].reshape(34 * N, C), wc2[dw, dh]) for dw in range(2) for dh in range(3)]
        v = relu(dots(pairs), 3, (34, N, C))
        if q == 0:
            v = bound(v, lf, 0, L)
        if q == N:
            v = bound(v, rt, L, C)
        put_rows(z2, q, v)

    def conv2_inner(q):
        pairs = [(y2[q + dw, dh + 2:dh + 32].reshape(30 * N, C), wc2[dw, dh]) for dw in range(2) for dh in range(3)]
        z2[q, 2:32] = finish(dots(pairs), 3, (30, N, C))

    def conv2_rest(first, last):
        pairs = []
        for dw in range(2):
            for dh in range(3):
                lhs = [y2[q + dw, h + dh:h + dh + 2].reshape(2 * N, C) for q in range(first, last) for h in (0, 32)]
                pairs.append((jnp.concatenate(lhs, axis=0), wc2[dw, dh]))
        v = relu(dots(pairs), 3, (last - first, 4, N, C))
        z2[first:last, 0:1] = bound(v[:, 0:1], up).astype(BF16)
        z2[first:last, 1:2] = v[:, 1:2].astype(BF16)
        z2[first:last, 32:33] = v[:, 2:3].astype(BF16)
        z2[first:last, 33:34] = bound(v[:, 3:4], dn).astype(BF16)

    down2(0)
    down2(N - 1)
    start(y2_cols)
    loop(1, 8, 7, down2)
    start(y2_rows[0])
    loop(8, N - 1, 7, down2)
    start(y2_rows[1])
    for q in range(3, 12):
        conv2_inner(q)
    for copies in (*y2_rows, y2_cols):
        finished(copies)
    for q in (0, 1, 2, 14, 15, N):
        conv2(q)
    for copy in loads[4:6]:
        copy.wait()

    def down3(k):
        pairs = []
        for dw in range(2):
            for dh in range(4):
                lhs = [z2[2 * k + e + dw, dh + 2 * i] for e in range(2) for i in range(N)]
                pairs.append((jnp.concatenate(lhs, axis=0), wd3[dh, 2 * dw:2 * dw + 2].reshape(C, C)))
        y3[pl.ds(2 * k + 1, 2), 1:17] = finish(dots(pairs), 4, (2, N, N, C))

    down3(0)
    down3(7)
    start(y3_cols)
    conv2_inner(12)
    conv2_inner(13)
    conv2_rest(3, 14)
    for k in range(1, 7):
        down3(k)
    start(y3_rows)

    def conv3(pair, slot):
        pairs = []
        for dw in range(3):
            for dh in range(3):
                lhs = [y3[dw:dw + N, i + dh].reshape(C, C) for i in pair]
                pairs.append((jnp.concatenate(lhs, axis=0), wc3[dh, dw]))
        res = jnp.maximum(dots(pairs) + biases[5:6, :], 0.0)
        for e, i in enumerate(pair):
            at = 2 * slot + e
            for j in range(N):
                for half in range(2):
                    row = (N * e + j) * N
                    turn[at, half, pl.ds(j, N, stride=PITCH), :] = res[row:row + N, half * L:half * L + L]
            for n in range(N):
                both = [turn[at, half, PITCH * n:PITCH * n + N, :] for half in range(2)]
                out_ref[n, i] = jnp.concatenate(both, axis=1).astype(BF16)

    def put_out(i, size, k):
        return pltpu.make_async_copy(out_ref.at[:, pl.ds(i, size)], out_hbm.at[:, pl.ds(i, size)], osem.at[k])

    finished(y3_cols)

    def conv3_inner(t, _):
        for e in range(3):
            i = 6 * t + 2 * e + 1
            conv3((i, i + 1), e)
        put_out(6 * t + 1, 6, t).start()
        return 0

    lax.fori_loop(0, 2, conv3_inner, 0)
    finished(y3_rows)
    last = [put_out(13, 2, 2), put_out(0, 1, 3), put_out(15, 1, 4)]
    conv3((13, 14), 0)
    last[0].start()
    conv3((0,), 1)
    last[1].start()
    conv3((15,), 2)
    last[2].start()
    for copy in (put_out(1, 6, 0), put_out(7, 6, 1), *last):
        copy.wait()


def hand_on(src, dst, held, isem, osem):
    parts = [pl.ds(2 * k, 2) for k in range(8)]
    reads = [pltpu.make_async_copy(src.at[p], held.at[p], isem.at[k]) for k, p in enumerate(parts)]
    writes = [pltpu.make_async_copy(held.at[p], dst.at[p], osem.at[k]) for k, p in enumerate(parts)]
    for copy in reads:
        copy.start()
    for read, write in zip(reads, writes):
        read.wait()
        write.start()
    for copy in writes:
        copy.wait()


def pack_down1(w_down1, wd1):
    for dh in range(2):
        blocks = []
        for ch in range(3):
            for u in range(4):
                across = []
                for eh in range(2):
                    for ew in range(2):
                        kh = 4 * dh + u - 2 * eh
                        if 0 <= kh < 4:
                            down = [w_down1[kh, ch].astype(F32), jnp.zeros((4 - 2 * ew, HALF), F32)]
                            across.append(jnp.concatenate(([jnp.zeros((2, HALF), F32)] if ew else []) + down, axis=0))
                        else:
                            across.append(jnp.zeros((8, HALF), F32))
                blocks.append(jnp.concatenate(across, axis=1))
        blocks.append(jnp.zeros((32, C), F32))
        wd1[L * dh:L * dh + L, :] = jnp.concatenate(blocks, axis=0).astype(BF16)


def pack_conv1(w_conv1, wc1):
    for dw in range(2):
        for mw in range(2):
            for dh in range(2):
                for mh in range(2):
                    across = []
                    for eh in range(2):
                        for ew in range(2):
                            kh, kw = 2 * dh + mh - eh, 2 * dw + mw - ew
                            inside = 0 <= kh < 3 and 0 <= kw < 3
                            across.append(w_conv1[kh, kw] if inside else jnp.zeros((HALF, HALF), BF16))
                    at = (2 * mh + mw) * HALF
                    wc1[dw, dh, at:at + HALF, :] = jnp.concatenate(across, axis=1)


def pack_stage2(w_down2, w_conv2, wd2, wc2):
    for dw in range(3):
        for mw in range(2):
            for dh in range(2):
                for mh in range(2):
                    at = (2 * mh + mw) * HALF
                    for ew in range(2):
                        kw = 2 * dw + mw - 2 * ew
                        value = w_down2[2 * dh + mh, kw] if 0 <= kw < 4 else jnp.zeros((HALF, L), BF16)
                        wd2[dw, dh, at:at + HALF, L * ew:L * ew + L] = value
    for dw in range(2):
        for mw in range(2):
            for kh in range(3):
                for ew in range(2):
                    kw = 2 * dw + mw - ew
                    value = w_conv2[kh, kw] if 0 <= kw < 3 else jnp.zeros((L, L), BF16)
                    wc2[dw, kh, L * mw:L * mw + L, L * ew:L * ew + L] = value


def solution(mesh):
    rows, cols = mesh.shape['row'], mesh.shape['col']

    def local(images, w_down1, b_down1, w_conv1, b_conv1, w_down2, b_down2, w_conv2, b_conv2, w_down3, b_down3, w_conv3, b_conv3):
        x = jnp.transpose(images, (0, 3, 1, 2))

        def act(w, h):
            return pltpu.VMEM((w, h, N, C), BF16)

        hbm = pl.BlockSpec(memory_space=pl.ANY)
        strip = pltpu.VMEM((12, 8, PIX), BF16)
        taps1 = jnp.transpose(w_down1, (0, 2, 1, 3))
        bias_rows = [b.reshape(1, -1) for b in (b_down1, b_conv1, b_down2, b_conv2, b_down3, b_conv3)]
        weight_in = [pltpu.VMEM(w.shape, BF16) for w in (taps1, w_conv1, w_down2, w_conv2)]
        weights = [pltpu.VMEM(shape, BF16) for shape in
                   ((C, C), (2, 2, C, C), (3, 2, C, C), (2, 3, C, C), w_down3.shape, w_conv3.shape)]
        dma = pltpu.SemaphoreType.DMA
        out = pl.pallas_call(
            functools.partial(body, rows, cols),
            out_shape=jax.ShapeDtypeStruct((N, N, N, C), BF16),
            in_specs=[hbm] * 13,
            out_specs=hbm,
            scratch_shapes=[pltpu.VMEM(b.shape, F32) for b in bias_rows] + [pltpu.VMEM((N, 3, L, L), BF16)] + weight_in + [pltpu.VMEM((N, 3, 8, L), BF16)] * 2
            + [pltpu.VMEM((3, PITCH * (L + N), L), F32), pltpu.VMEM((12, 144, PIX), F32), pltpu.VMEM((34, 2, N, L), BF16)] + [strip] * 4
            + [act(34, 34), act(33, 33), act(18, 36), act(17, 34), act(18, 18)] + weights
            + [pltpu.VMEM((8, C), F32), pltpu.VMEM((6, 2, PITCH * N, L), F32), act(N, N), dma((28,)), dma((28,)), dma((13,)), dma((5,))],
            compiler_params=pltpu.CompilerParams(collective_id=0, has_side_effects=True, vmem_limit_bytes=66_000_000),
            name='encoder',
        )(x, taps1, w_conv1, w_down2, w_conv2, w_down3, w_conv3, *bias_rows)
        return pl.pallas_call(
            hand_on,
            out_shape=jax.ShapeDtypeStruct(out.shape, BF16),
            in_specs=[hbm],
            out_specs=hbm,
            scratch_shapes=[act(N, N), dma((8,)), dma((8,))],
            name='hand_on',
        )(out)

    tile_spec = P('batch', 'row', 'col', None)
    return jax.shard_map(local, mesh=mesh, in_specs=(tile_spec,) + (P(),) * 12, out_specs=tile_spec, check_vma=False)
```

```python
import functools

import jax
import jax.numpy as jnp
from jax import lax
from jax.experimental import pallas as pl
from jax.experimental.pallas import tpu as pltpu
from jax.sharding import PartitionSpec as P

MESH = pl.DeviceIdType.MESH
F32 = jnp.float32
BF16 = jnp.bfloat16

N = 16
L = 128
C = 256
PIX = 640
HALF = 64
PITCH = 17


def body(rows, cols, x_hbm, w_down1_hbm, w_conv1_hbm, w_down2_hbm, w_conv2_hbm, w_down3, w_conv3, *refs):
    b_hbm, out_hbm, bs = refs[:6], refs[6], refs[7:13]
    (x_ref, w_down1, w_conv1, w_down2, w_conv2, top, bot, xs, tt, kept, send_l, send_r, recv_l, recv_r, y1, z1, y2, z2,
     y3, wd1, wc1, wd2, wc2, wd3, wc3, biases, turn, out_ref, ssem, rsem, wsem, osem) = refs[13:]
    r = lax.axis_index('row')
    c = lax.axis_index('col')
    has_up, has_dn = r > 0, r < rows - 1
    has_lf, has_rt = c > 0, c < cols - 1

    loads = [pltpu.make_async_copy(src, dst, wsem.at[k]) for k, (src, dst) in enumerate((
        (x_hbm, x_ref), (w_conv1_hbm, w_conv1), (w_down2_hbm, w_down2), (w_conv2_hbm, w_conv2), (w_down3, wd3), (w_conv3, wc3),
        (w_down1_hbm, w_down1), *zip(b_hbm, bs)))]

    neighbours = []
    for dr in (-1, 0, 1):
        for dc in (-1, 0, 1):
            if dr == 0 and dc == 0:
                continue
            there = None
            if dr:
                there = has_up if dr < 0 else has_dn
            if dc:
                side = has_lf if dc < 0 else has_rt
                there = side if there is None else jnp.logical_and(there, side)
            neighbours.append((dr, dc, there))

    def device(dr, dc):
        return {'row': r + dr, 'col': c + dc}

    barrier = pltpu.get_barrier_semaphore()
    for dr, dc, there in neighbours:
        if dr and dc:
            continue

        @pl.when(there)
        def _():
            pl.semaphore_signal(barrier, inc=1, device_id=device(dr, dc), device_id_type=MESH)
    for copy in loads:
        copy.start()
    pl.semaphore_wait(barrier, sum(t.astype(jnp.int32) for t in (has_up, has_dn, has_lf, has_rt)))

    def remote(src, dst, k, dr, dc):
        return pltpu.make_async_remote_copy(src_ref=src, dst_ref=dst, send_sem=ssem.at[k], recv_sem=rsem.at[k],
                                            device_id=device(dr, dc), device_id_type=MESH)

    to_dn = remote(x_ref.at[:, :, L - 8:L], top, 0, 1, 0)
    to_up = remote(x_ref.at[:, :, 0:8], bot, 1, -1, 0)
    loads[0].wait()

    @pl.when(has_dn)
    def _():
        to_dn.start()

    @pl.when(has_up)
    def _():
        to_up.start()

    up, dn, lf, rt = (jnp.where(there, jnp.inf, 0.0).astype(F32) for there in (has_up, has_dn, has_lf, has_rt))

    def clear(ref, there, index):
        @pl.when(jnp.logical_not(there))
        def _():
            ref[index] = jnp.zeros_like(ref[index])

    every = slice(None)
    clear(top, has_up, (every,))
    clear(bot, has_dn, (every,))
    clear(recv_l, has_lf, (every,))
    clear(recv_r, has_rt, (every,))
    for ref, step, last in ((y2, 2, 34), (y3, 1, N + 1)):
        clear(ref, has_up, (every, slice(0, step)))
        clear(ref, has_dn, (every, slice(last, last + step)))
        clear(ref, has_lf, (slice(0, 1),))
        clear(ref, has_rt, (slice(N + 1, N + 2),))
    for copy in loads[6:]:
        copy.wait()
    pack_down1(w_down1, wd1)
    for k, b in enumerate(bs):
        biases[k:k + 1, :] = jnp.concatenate([b[...]] * (C // b.shape[1]), axis=1)

    def gather(ch, src, h, size):
        for n in range(N):
            xs[ch, pl.ds(PITCH * (h + 8) + n, size, stride=PITCH), :] = src[n, ch].astype(F32)

    def put(ch, g):
        for u in range(4):
            pieces = []
            for k in range(8):
                at = PITCH * (32 * g + u + 3 + 4 * k)
                pieces.append(xs[ch, at:at + N, :] if at < PITCH * (L + N) else jnp.zeros((N, L), F32))
            t = jnp.transpose(jnp.concatenate(pieces, axis=0))
            cu = ch * 4 + u
            lanes = slice(g * L, g * L + L)
            tt[cu, 5:5 + L, lanes] = t
            send_l[cu, :, lanes] = t[0:8].astype(BF16)
            send_r[cu, :, lanes] = t[L - 8:L].astype(BF16)

    def inner(ch, _):
        gather(ch, x_ref, 0, L)
        for g in (1, 2, 3):
            put(ch, g)
        return 0

    lax.fori_loop(0, 3, inner, 0)

    def dots(pairs):
        acc = None
        for lhs, w in pairs:
            d = jnp.dot(lhs, w, preferred_element_type=F32)
            acc = d if acc is None else acc + d
        return acc

    def relu(acc, k, shape):
        return jnp.maximum(acc + biases[k:k + 1, :], 0.0).reshape(shape)

    def finish(acc, k, shape):
        return relu(acc, k, shape).astype(BF16)

    def bound(v, inside, first=0, last=C):
        parts = [v[..., :first], jnp.minimum(v[..., first:last], inside), v[..., last:]]
        return jnp.concatenate([p for p in parts if p.shape[-1]], axis=-1)

    def put_rows(ref, w, v, first=(0, C), last=(0, C)):
        h = v.shape[0]
        ref[w, 0:1] = bound(v[0:1], up, *first).astype(BF16)
        ref[w, 1:h - 1] = v[1:h - 1].astype(BF16)
        ref[w, h - 1:h] = bound(v[h - 1:h], dn, *last).astype(BF16)

    def window(k, e, lanes):
        size = sum(last - first for first, last in lanes)
        win = [tt[:, 8 * k:8 * k + N, first:last][:, 4 * e:4 * e + 8].reshape(96, last - first) for first, last in lanes]
        xt = jnp.transpose(jnp.concatenate(win, axis=1).astype(BF16))
        return jnp.concatenate([xt, jnp.zeros((size, L - 96), BF16)], axis=1)

    def down1(k):
        m = 34 * N
        for e in range(2):
            xb = window(k, e, [(0, PIX)])
            lhs = jnp.concatenate([xb[0:m], xb[N:N + m]], axis=1)
            v = relu(dots([(lhs, wd1[...])]), 0, (34, N, C))
            if 2 * k + e in (0, 33):
                v = jnp.minimum(v, rt if k else lf)
            put_rows(y1, 2 * k + e, v)

    def down1_inner(k):
        m = 23 * N
        for e in range(2):
            xb = window(k, e, [(L, 4 * L)])
            kept[2 * k + e, 0] = xb[0:N]
            kept[2 * k + e, 1] = xb[m:m + N]
            lhs = jnp.concatenate([xb[0:m], xb[N:N + m]], axis=1)
            y1[2 * k + e, 8:31] = finish(dots([(lhs, wd1[...])]), 0, (23, N, C))

    def down1_outer(k):
        lhs = []
        for e in range(2):
            xb = window(k, e, [(0, L), (4 * L, PIX)])
            this = jnp.concatenate([xb[0:L], kept[2 * k + e, 1], xb[L:L + 2 * N]], axis=0)
            below = jnp.concatenate([xb[N:L], kept[2 * k + e, 0], xb[L:L + 3 * N]], axis=0)
            lhs.append(jnp.concatenate([this, below], axis=1))
        v = relu(dots([(jnp.concatenate(lhs, axis=0), wd1[...])]), 0, (2, 11, N, C))
        both = slice(2 * k, 2 * k + 2)
        y1[both, 0:1] = bound(v[:, 0:1], up).astype(BF16)
        y1[both, 1:8] = v[:, 1:8].astype(BF16)
        y1[both, 31:33] = v[:, 8:10].astype(BF16)
        y1[both, 33:34] = bound(v[:, 10:11], dn).astype(BF16)

    for k in range(1, N):
        down1_inner(k)

    @pl.when(has_up)
    def _():
        to_up.wait_send()
        to_dn.wait_recv()

    @pl.when(has_dn)
    def _():
        to_dn.wait_send()
        to_up.wait_recv()

    def outer(ch, _):
        gather(ch, top, -8, 8)
        gather(ch, bot, L, 8)
        for g in (0, 4):
            put(ch, g)
        return 0

    lax.fori_loop(0, 3, outer, 0)

    to_lf = remote(send_l, recv_r, 2, 0, -1)
    to_rt = remote(send_r, recv_l, 3, 0, 1)

    @pl.when(has_lf)
    def _():
        to_lf.start()

    @pl.when(has_rt)
    def _():
        to_rt.start()

    def loop(start, stop, unroll, step):
        assert (stop - start) % unroll == 0

        def run(t, _):
            for e in range(unroll):
                step(start + t * unroll + e)
            return 0

        lax.fori_loop(0, (stop - start) // unroll, run, 0)

    def conv1(b):
        pairs = [(y1[b + dw, dh:dh + 33].reshape(33 * N, C), wc1[dw, dh]) for dw in range(2) for dh in range(2)]
        v = relu(dots(pairs), 1, (33, N, C))
        if isinstance(b, int):
            for half in (0, L):
                if b == 0:
                    v = bound(v, lf, half, half + HALF)
                if b == 32:
                    v = bound(v, rt, half + HALF, half + L)
        put_rows(z1, b, v, (0, L), (L, C))

    for copy in loads[1:4]:
        copy.wait()
    pack_conv1(w_conv1, wc1)
    for k in range(1, N):
        down1_outer(k)
    loop(2, 18, 16, conv1)

    @pl.when(has_lf)
    def _():
        to_lf.wait_send()
        to_rt.wait_recv()

    @pl.when(has_rt)
    def _():
        to_rt.wait_send()
        to_lf.wait_recv()

    tt[:, 0:5, :] = recv_l[...].astype(F32)[:, 3:8]
    tt[:, 5 + L:13 + L, :] = recv_r[...].astype(F32)
    down1(0)
    down1(N)
    pack_stage2(w_down2, w_conv2, wd2, wc2)
    for b in (*range(18, 33), 0, 1):
        conv1(b)

    def edge(d, around, size, step):
        first, last = around, around + size
        if d == 0:
            return slice(first, last), slice(first, last)
        if d > 0:
            return slice(last - step, last), slice(first - step, first)
        return slice(first, first + step), slice(last, last + step)

    def start(copies):
        for copy, there, _ in copies:
            @pl.when(there)
            def _():
                copy.start()

    def finished(copies):
        for copy, there, back in copies:
            @pl.when(there)
            def _():
                copy.wait_send()
                back.wait_recv()

    def exchange(ref, k0, w_axis, h_axis, wanted):
        made = {}
        for k, (dr, dc, there) in enumerate(neighbours):
            if wanted(dr, dc):
                (ws, wd), (hs, hd) = edge(dc, *w_axis), edge(dr, *h_axis)
                made[k] = (remote(ref.at[ws, hs], ref.at[wd, hd], k0 + k, dr, dc), there)
        return [(copy, there, made[7 - k][0]) for k, (copy, there) in made.items()]

    def sideways(dr, dc):
        return dc != 0

    def upright(dr, dc):
        return dc == 0

    y2_cols = exchange(y2, 4, (1, N, 1), (2, 32, 2), sideways)
    y2_rows = [exchange(y2, k0, (w0, 8, 1), (2, 32, 2), upright) for k0, w0 in ((4, 1), (12, 9))]
    y3_cols = exchange(y3, 20, (1, N, 1), (1, N, 1), sideways)
    y3_rows = exchange(y3, 20, (1, N, 1), (1, N, 1), upright)

    def down2(p):
        pairs = [(z1[2 * p + dw, dh:dh + 32].reshape(32 * N, C), wd2[dw, dh]) for dw in range(3) for dh in range(2)]
        y2[p + 1, 2:34] = finish(dots(pairs), 2, (32, N, C))

    def conv2(q):
        pairs = [(y2[q + dw, dh:dh + 34].reshape(34 * N, C), wc2[dw, dh]) for dw in range(2) for dh in range(3)]
        v = relu(dots(pairs), 3, (34, N, C))
        if q == 0:
            v = bound(v, lf, 0, L)
        if q == N:
            v = bound(v, rt, L, C)
        put_rows(z2, q, v)

    def conv2_inner(q):
        pairs = [(y2[q + dw, dh + 2:dh + 32].reshape(30 * N, C), wc2[dw, dh]) for dw in range(2) for dh in range(3)]
        z2[q, 2:32] = finish(dots(pairs), 3, (30, N, C))

    def conv2_rest(first, last):
        pairs = []
        for dw in range(2):
            for dh in range(3):
                lhs = [y2[q + dw, h + dh:h + dh + 2].reshape(2 * N, C) for q in range(first, last) for h in (0, 32)]
                pairs.append((jnp.concatenate(lhs, axis=0), wc2[dw, dh]))
        v = relu(dots(pairs), 3, (last - first, 4, N, C))
        z2[first:last, 0:1] = bound(v[:, 0:1], up).astype(BF16)
        z2[first:last, 1:2] = v[:, 1:2].astype(BF16)
        z2[first:last, 32:33] = v[:, 2:3].astype(BF16)
        z2[first:last, 33:34] = bound(v[:, 3:4], dn).astype(BF16)

    down2(0)
    down2(N - 1)
    start(y2_cols)
    loop(1, 8, 7, down2)
    start(y2_rows[0])
    loop(8, N - 1, 7, down2)
    start(y2_rows[1])
    for q in range(3, 12):
        conv2_inner(q)
    for copies in (*y2_rows, y2_cols):
        finished(copies)
    for q in (0, 1, 2, 14, 15, N):
        conv2(q)
    for copy in loads[4:6]:
        copy.wait()

    def down3(k):
        pairs = []
        for dw in range(2):
            for dh in range(4):
                lhs = [z2[2 * k + e + dw, dh + 2 * i] for e in range(2) for i in range(N)]
                pairs.append((jnp.concatenate(lhs, axis=0), wd3[dh, 2 * dw:2 * dw + 2].reshape(C, C)))
        y3[pl.ds(2 * k + 1, 2), 1:17] = finish(dots(pairs), 4, (2, N, N, C))

    down3(0)
    down3(7)
    start(y3_cols)
    conv2_inner(12)
    conv2_inner(13)
    conv2_rest(3, 14)
    for k in range(1, 7):
        down3(k)
    start(y3_rows)

    def conv3(pair, slot):
        pairs = []
        for dw in range(3):
            for dh in range(3):
                lhs = [y3[dw:dw + N, i + dh].reshape(C, C) for i in pair]
                pairs.append((jnp.concatenate(lhs, axis=0), wc3[dh, dw]))
        res = jnp.maximum(dots(pairs) + biases[5:6, :], 0.0)
        for e, i in enumerate(pair):
            at = 2 * slot + e
            for j in range(N):
                for half in range(2):
                    row = (N * e + j) * N
                    turn[at, half, pl.ds(j, N, stride=PITCH), :] = res[row:row + N, half * L:half * L + L]
            for n in range(N):
                both = [turn[at, half, PITCH * n:PITCH * n + N, :] for half in range(2)]
                out_ref[n, i] = jnp.concatenate(both, axis=1).astype(BF16)

    def put_out(i, size, k):
        return pltpu.make_async_copy(out_ref.at[:, pl.ds(i, size)], out_hbm.at[:, pl.ds(i, size)], osem.at[k])

    finished(y3_cols)

    def conv3_inner(t, _):
        for e in range(3):
            i = 6 * t + 2 * e + 1
            conv3((i, i + 1), e)
        put_out(6 * t + 1, 6, t).start()
        return 0

    lax.fori_loop(0, 2, conv3_inner, 0)
    finished(y3_rows)
    last = [put_out(13, 2, 2), put_out(0, 1, 3), put_out(15, 1, 4)]
    conv3((13, 14), 0)
    last[0].start()
    conv3((0,), 1)
    last[1].start()
    conv3((15,), 2)
    last[2].start()
    for copy in (put_out(1, 6, 0), put_out(7, 6, 1), *last):
        copy.wait()


def hand_on(src, dst, held, isem, osem):
    parts = [pl.ds(k, 1) for k in range(N)]
    reads = [pltpu.make_async_copy(src.at[p], held.at[p], isem.at[k]) for k, p in enumerate(parts)]
    writes = [pltpu.make_async_copy(held.at[p], dst.at[p], osem.at[k]) for k, p in enumerate(parts)]
    for copy in reads:
        copy.start()
    for read, write in zip(reads, writes):
        read.wait()
        write.start()
    for copy in writes:
        copy.wait()


def pack_down1(w_down1, wd1):
    for dh in range(2):
        blocks = []
        for ch in range(3):
            for u in range(4):
                across = []
                for eh in range(2):
                    for ew in range(2):
                        kh = 4 * dh + u - 2 * eh
                        if 0 <= kh < 4:
                            down = [w_down1[kh, ch].astype(F32), jnp.zeros((4 - 2 * ew, HALF), F32)]
                            across.append(jnp.concatenate(([jnp.zeros((2, HALF), F32)] if ew else []) + down, axis=0))
                        else:
                            across.append(jnp.zeros((8, HALF), F32))
                blocks.append(jnp.concatenate(across, axis=1))
        blocks.append(jnp.zeros((32, C), F32))
        wd1[L * dh:L * dh + L, :] = jnp.concatenate(blocks, axis=0).astype(BF16)


def pack_conv1(w_conv1, wc1):
    for dw in range(2):
        for mw in range(2):
            for dh in range(2):
                for mh in range(2):
                    across = []
                    for eh in range(2):
                        for ew in range(2):
                            kh, kw = 2 * dh + mh - eh, 2 * dw + mw - ew
                            inside = 0 <= kh < 3 and 0 <= kw < 3
                            across.append(w_conv1[kh, kw] if inside else jnp.zeros((HALF, HALF), BF16))
                    at = (2 * mh + mw) * HALF
                    wc1[dw, dh, at:at + HALF, :] = jnp.concatenate(across, axis=1)


def pack_stage2(w_down2, w_conv2, wd2, wc2):
    for dw in range(3):
        for mw in range(2):
            for dh in range(2):
                for mh in range(2):
                    at = (2 * mh + mw) * HALF
                    for ew in range(2):
                        kw = 2 * dw + mw - 2 * ew
                        value = w_down2[2 * dh + mh, kw] if 0 <= kw < 4 else jnp.zeros((HALF, L), BF16)
                        wd2[dw, dh, at:at + HALF, L * ew:L * ew + L] = value
    for dw in range(2):
        for mw in range(2):
            for kh in range(3):
                for ew in range(2):
                    kw = 2 * dw + mw - ew
                    value = w_conv2[kh, kw] if 0 <= kw < 3 else jnp.zeros((L, L), BF16)
                    wc2[dw, kh, L * mw:L * mw + L, L * ew:L * ew + L] = value


def solution(mesh):
    rows, cols = mesh.shape['row'], mesh.shape['col']

    def local(images, w_down1, b_down1, w_conv1, b_conv1, w_down2, b_down2, w_conv2, b_conv2, w_down3, b_down3, w_conv3, b_conv3):
        x = jnp.transpose(images, (0, 3, 1, 2))

        def act(w, h):
            return pltpu.VMEM((w, h, N, C), BF16)

        hbm = pl.BlockSpec(memory_space=pl.ANY)
        strip = pltpu.VMEM((12, 8, PIX), BF16)
        taps1 = jnp.transpose(w_down1, (0, 2, 1, 3))
        bias_rows = [b.reshape(1, -1) for b in (b_down1, b_conv1, b_down2, b_conv2, b_down3, b_conv3)]
        weight_in = [pltpu.VMEM(w.shape, BF16) for w in (taps1, w_conv1, w_down2, w_conv2)]
        weights = [pltpu.VMEM(shape, BF16) for shape in
                   ((C, C), (2, 2, C, C), (3, 2, C, C), (2, 3, C, C), w_down3.shape, w_conv3.shape)]
        dma = pltpu.SemaphoreType.DMA
        out = pl.pallas_call(
            functools.partial(body, rows, cols),
            out_shape=jax.ShapeDtypeStruct((N, N, N, C), BF16),
            in_specs=[hbm] * 13,
            out_specs=hbm,
            scratch_shapes=[pltpu.VMEM(b.shape, F32) for b in bias_rows] + [pltpu.VMEM((N, 3, L, L), BF16)] + weight_in + [pltpu.VMEM((N, 3, 8, L), BF16)] * 2
            + [pltpu.VMEM((3, PITCH * (L + N), L), F32), pltpu.VMEM((12, 144, PIX), F32), pltpu.VMEM((34, 2, N, L), BF16)] + [strip] * 4
            + [act(34, 34), act(33, 33), act(18, 36), act(17, 34), act(18, 18)] + weights
            + [pltpu.VMEM((8, C), F32), pltpu.VMEM((6, 2, PITCH * N, L), F32), act(N, N), dma((28,)), dma((28,)), dma((13,)), dma((5,))],
            compiler_params=pltpu.CompilerParams(collective_id=0, has_side_effects=True, vmem_limit_bytes=66_000_000),
            name='encoder',
        )(x, taps1, w_conv1, w_down2, w_conv2, w_down3, w_conv3, *bias_rows)
        return pl.pallas_call(
            hand_on,
            out_shape=jax.ShapeDtypeStruct(out.shape, BF16),
            in_specs=[hbm],
            out_specs=hbm,
            scratch_shapes=[act(N, N), dma((N,)), dma((N,))],
            name='hand_on',
        )(out)

    tile_spec = P('batch', 'row', 'col', None)
    return jax.shard_map(local, mesh=mesh, in_specs=(tile_spec,) + (P(),) * 12, out_specs=tile_spec, check_vma=False)
```
